512 devices in a mesh: dp: 128 (over z, y, core), group: 4 (over x).
Axes of the slice: x: 4, y: 8, z: 8, core: 2. Of those that a mesh axis runs over, the one named last changes fastest.
Arguments:
- features: bfloat16 [65536, 512], P(('dp', 'group')), may hold values from -6 to 6
- head_weight: bfloat16 [512, 512], replicated, may hold values from -0.25 to 0.25
- owner_of_image: int32 [65536, 1], P(('dp', 'group')), may hold values from 0 to 127; in each aligned block of 128 rows (0 to 127, 128 to 255, ...) at most 2 rows name the same one
- class_slot: int32 [65536], P(('dp', 'group')), may hold values from 0 to 49
- is_query: int32 [65536], P(('dp', 'group')), may hold values 0 or 1
- episode_ways: int32 [512], P(('dp', 'group')), may hold values from 5 to 50
Outputs:
- grad_features: bfloat16 [65536, 512], P(('dp', 'group'))
- grad_weight: float32 [512, 512], replicated
- losses: float32 [512], P(('dp', 'group'))
The draws below stay inside these ranges and needn't reach their ends.
Inputs may be any that keep to these rules, and one draw needn't show every extreme that they name: `owner_of_image`: among the rows of one device at most 2 name any one owner, a bound that some block reaches.
All inputs are finite; a program needn't handle non-finite values. No bound on the sum of `is_query` on one device may be relied on, other than what follows from the above.
Results may differ from the reference program's by a relative error of at most 0.0037.
The reference program's roundings to bfloat16 on the way count: a program that leaves them out, or rounds other values in their place, can miss the bound.
Values may be sent and summed in bfloat16 or wider, within the bound.
A program may use at most 64 MiB of HBM per device.

```python
import math
import jax
import jax.numpy as jnp
import numpy as np
from jax import lax

D = 512
WAYS_MAX = 50
ROWS_DEV = 128
EP_DEV = 1
CAP = 2
IMAGES = 65536
EPISODES = 512
N_DP = 128
N_GROUP = 4


def touch_ends(array, rng, least, top_value):
    longest = array.shape.index(max(array.shape))
    spots = []
    for shift in (0, 1):
        where = [jax.random.randint(jax.random.fold_in(rng, axis), (), 0, length) for axis, length in enumerate(array.shape)]
        where[longest] = (where[longest] + shift) % array.shape[longest]
        spots.append(tuple(where))
    return array.at[spots[0]].set(least).at[spots[1]].set(top_value)


def block_levels(stream_key, extent, split, least, high):
    level, own = 1.0, jax.random.fold_in(stream_key, 6)
    for axis_at, shards_of in split:
        draws = jnp.exp(jax.random.uniform(jax.random.fold_in(own, axis_at), (shards_of,), jnp.float32, least / len(split), high / len(split)))
        level = level * jnp.repeat(draws, extent[axis_at] // shards_of).reshape([-1 if axis == axis_at else 1 for axis in range(len(extent))])
    return level


def routed_block(stream_key, own, number, rows, number_of, top, bound, skew):
    ranking = jax.random.permutation(stream_key, number_of)
    packed, common = portions_of(number_of, rows * top, bound, skew, True), portions_of(number_of, rows * top, bound, skew, False)
    places = jnp.arange(number_of)

    def named(sizes, rotation):
        used = int((sizes > 0).sum())
        fixed = max(1, used // 4)
        moved = fixed + (places - fixed + rotation * (used - fixed)) % max(1, number_of - fixed)
        return jnp.zeros((number_of,), jnp.int32).at[ranking[jnp.where(places < fixed, places, moved)]].set(jnp.asarray(sizes, jnp.int32))

    sizes = jnp.where(number % 4 == 0, named(packed, number // 4), named(common, number - number // 4 - 1))
    mixed = jax.random.permutation(jax.random.fold_in(own, 3), number_of)
    source_of, taker = mixed[0:number_of // 2 * 2:2], mixed[1:number_of // 2 * 2:2]
    room = jnp.minimum(sizes[source_of] - 1, bound - sizes[taker]) // 2
    room = jnp.where((source_of == ranking[0]) | (taker == ranking[0]) | (sizes[taker] == 0), 0, jnp.maximum(room, 0))
    moved = jax.random.randint(jax.random.fold_in(own, 4), (number_of // 2,), 0, 1 << 20) % (room + 1)
    sizes = sizes.at[source_of].add(-moved).at[taker].add(moved)
    labels = jnp.searchsorted(jnp.cumsum(sizes), jnp.arange(rows * top), side="right").astype(jnp.int32)
    grid = labels.reshape(top, rows).T
    grid = grid[jax.random.permutation(jax.random.fold_in(own, 1), rows)]
    rotation = jax.random.randint(jax.random.fold_in(own, 2), (rows, 1), 0, top)
    return jnp.take_along_axis(grid, (jnp.arange(top)[None, :] + rotation) % top, axis=1)


def portions_of(number_of, total, most, lean, full):
    weights = [(1 << 20) // math.isqrt(grade ** lean) + 1 for grade in range(1, number_of + 1)]
    largest = most if full else min(most, max(-(-total // number_of), total * weights[0] // sum(weights)))
    least = 1 if total - largest >= number_of - 1 else 0
    given, rest = [largest] + [least] * (number_of - 1), total - largest - least * (number_of - 1)
    while rest > 0:
        free = [i for i in range(1, number_of) if given[i] < largest] or [i for i in range(1, number_of) if given[i] < most]
        mass, budget = sum([weights[i] for i in free]), rest
        for i in free:
            addition = min(most - given[i], max(1, budget * weights[i] // mass), rest)
            given[i] = given[i] + addition
            rest = rest - addition
    return np.array(given)


def normal_values(stream_key, shape, deviation, bound, shards=(), kind=jnp.bfloat16):
    values = deviation * jax.random.normal(stream_key, shape, jnp.float32)
    if shards:
        values = values * block_levels(stream_key, shape, shards, -0.22, 0.18)
    return jnp.clip(values, -bound, bound).astype(kind)


def setup_inputs(seed: int = 0) -> dict:
    arg_keys = jax.random.split(jax.random.key(seed), 7)
    features = normal_values(arg_keys[0], (IMAGES, D), 1.0, 6.0, ((0, 512),))
    head_weight = normal_values(arg_keys[1], (D, D), D ** -0.5, 0.25)
    owner_of_image_keys = jax.random.split(jax.random.fold_in(arg_keys[2], 1), IMAGES // ROWS_DEV)
    owner_of_image_turns = jax.random.permutation(jax.random.fold_in(arg_keys[2], 3), IMAGES // ROWS_DEV)
    owner_of_image = jax.vmap(lambda own, number: routed_block(jax.random.fold_in(arg_keys[2], 2), own, number, ROWS_DEV, N_DP, 1, CAP, 2))(owner_of_image_keys, owner_of_image_turns).reshape((IMAGES, 1))
    class_slot = touch_ends(jax.random.randint(arg_keys[3], (IMAGES,), 0, EP_DEV * WAYS_MAX), jax.random.fold_in(arg_keys[3], 1), 0, (EP_DEV * WAYS_MAX) - 1).astype(jnp.int32)
    is_query = touch_ends((jax.random.randint(arg_keys[4], (IMAGES,), 0, 2) < 1).astype(jnp.int32), jax.random.fold_in(arg_keys[4], 1), 0, 1)
    episode_ways = touch_ends(jax.random.randint(arg_keys[5], (EPISODES,), 5, WAYS_MAX + 1), jax.random.fold_in(arg_keys[5], 1), 5, WAYS_MAX).astype(jnp.int32)
    return dict(features=features, head_weight=head_weight, owner_of_image=owner_of_image, class_slot=class_slot, is_query=is_query, episode_ways=episode_ways)


def episode_losses(embeds, codes, ways_table):
    count_ep = ways_table.shape[0]
    is_live = codes > 0
    code_value = jnp.maximum(codes - 1, 0)
    query_rows = is_live & (code_value % 2 == 1)
    support_rows = is_live & (code_value % 2 == 0)
    slot_value = code_value // 2
    episode = slot_value // WAYS_MAX
    raw_class = slot_value % WAYS_MAX
    episode_hot = episode[:, None] == jnp.arange(count_ep, dtype=jnp.int32)[None, :]
    row_ways = lax.optimization_barrier(jnp.sum(jnp.where(episode_hot, ways_table[None, :], 0), axis=1))
    label_id = episode * WAYS_MAX + raw_class % row_ways
    classes = jnp.arange(count_ep * WAYS_MAX, dtype=jnp.int32)
    class_hot = label_id[:, None] == classes[None, :]
    support_hot = (class_hot & support_rows[:, None]).astype(jnp.float32)
    counts = lax.optimization_barrier(jnp.sum(support_hot, axis=0))
    class_sums = jnp.dot(support_hot.T, embeds, precision=lax.Precision.HIGHEST)
    prototypes = class_sums / jnp.maximum(counts, 1.0)[:, None]
    class_ways = jnp.repeat(ways_table, WAYS_MAX)
    class_valid = classes % WAYS_MAX < class_ways
    allowed = (episode[:, None] == (classes // WAYS_MAX)[None, :]) & class_valid[None, :]
    cross_term = jnp.dot(embeds, prototypes.T, precision=lax.Precision.HIGHEST)
    distance = lax.optimization_barrier(jnp.sum(embeds * embeds, axis=1))[:, None] - 2.0 * cross_term + lax.optimization_barrier(jnp.sum(prototypes * prototypes, axis=1))[None, :]
    scores = -distance * D ** (-0.5)
    masked = jnp.where(allowed, scores, -1e+30)
    row_max = lax.optimization_barrier(jnp.max(masked, axis=1, keepdims=True))
    log_total = row_max[:, 0] + jnp.log(lax.optimization_barrier(jnp.sum(jnp.exp(masked - row_max), axis=1)))
    picked = lax.optimization_barrier(jnp.sum(jnp.where(class_hot, scores, 0.0), axis=1))
    per_query = jnp.where(query_rows, log_total - picked, 0.0)
    hot_float = episode_hot.astype(jnp.float32)
    query_count = lax.optimization_barrier(jnp.sum(hot_float * query_rows[:, None].astype(jnp.float32), axis=0))
    return lax.optimization_barrier(jnp.sum(hot_float * per_query[:, None], axis=0)) / jnp.maximum(query_count, 1.0)

def reference(features, head_weight, owner_of_image, class_slot, is_query, episode_ways):
    devices = N_DP * N_GROUP
    capacity = 2 * ROWS_DEV // N_DP
    slot_count = N_DP * capacity
    embeds = jnp.dot(features, head_weight, preferred_element_type=jnp.float32).astype(jnp.bfloat16)
    target = owner_of_image[:, 0].reshape(devices, ROWS_DEV)
    one_hot = (target[:, :, None] == jnp.arange(N_DP, dtype=jnp.int32)[None, None, :]).astype(jnp.int32)
    before = jnp.cumsum(one_hot, axis=1) - one_hot
    position = lax.optimization_barrier(jnp.sum(one_hot * before, axis=2))
    device_ids = jnp.arange(devices, dtype=jnp.int32)
    source = device_ids // N_GROUP
    group_id = device_ids % N_GROUP
    owner = target * N_GROUP + group_id[:, None]
    place = (owner * slot_count + source[:, None] * capacity + position).reshape(-1)
    codes = class_slot * 2 + is_query + 1
    table = jnp.zeros((devices * slot_count,), jnp.int32).at[place].set(jnp.arange(IMAGES, dtype=jnp.int32) + 1)
    table = table.reshape(devices, slot_count)

    def per_owner(inputs):
        index_row, ways_row = inputs
        is_live = index_row > 0
        pick_row = jnp.maximum(index_row - 1, 0)
        rows = jnp.where(is_live[:, None], embeds[pick_row].astype(jnp.float32), 0.0)
        code_row = jnp.where(is_live, codes[pick_row], 0)
        values, pull = jax.vjp(lambda e: episode_losses(e, code_row, ways_row), rows)
        grads = pull(jnp.ones_like(values))[0].astype(jnp.bfloat16)
        return (grads, values)
    grads, losses = lax.map(per_owner, (table, episode_ways.reshape(devices, EP_DEV)))
    grad_rows = grads.reshape(-1, D)[place]
    grad_features = lax.dot_general(grad_rows, head_weight, (((1,), (1,)), ((), ())), preferred_element_type=jnp.float32).astype(jnp.bfloat16)
    grad_weight = lax.dot_general(features, grad_rows, (((0,), (0,)), ((), ())), preferred_element_type=jnp.float32)
    return (grad_features, grad_weight, losses.reshape(-1))
```

```python
import functools

import jax
import jax.numpy as jnp
from jax import lax
from jax.experimental import pallas as pl
from jax.experimental.pallas import tpu as pltpu
from jax.sharding import PartitionSpec as P

D = 512
WAYS_MAX = 50
CLASSES = 64
CAP = 2
LANES = 128
MESH = pl.DeviceIdType.MESH
F32 = jnp.float32
BF16 = jnp.bfloat16
I32 = jnp.int32


def dot(a, b, ca, cb):
    return lax.dot_general(a, b, (((ca,), (cb,)), ((), ())), preferred_element_type=F32)


def iota(shape, dim):
    return lax.broadcasted_iota(I32, shape, dim)


def three_parts(x):
    hi = x.astype(BF16)
    rest = x - hi.astype(F32)
    mid = rest.astype(BF16)
    low = (rest - mid.astype(F32)).astype(BF16)
    return hi, mid, low


def to_lanes(column):
    n = column.shape[0]
    same = iota((n, n), 0) == iota((n, n), 1)
    return jnp.sum(jnp.where(same, column, 0.0), axis=0, keepdims=True)


def to_sublanes(row):
    n = row.shape[1]
    same = iota((n, n), 0) == iota((n, n), 1)
    return jnp.sum(jnp.where(same, row, 0.0), axis=1, keepdims=True)


def episode(rows, codes, ways, weight):
    count = rows.shape[0]
    embeds = dot(rows, weight, 1, 0).astype(BF16)
    wide = embeds.astype(F32)
    code = codes.astype(I32)
    value = jnp.maximum(code - 1, 0)
    live = code > 0
    odd = lax.rem(value, 2) == 1
    query = (live & odd).astype(F32)
    label = lax.div(value, 2)
    for factor in (8, 4, 2, 1):
        label = jnp.where(label >= factor * ways, label - factor * ways, label)
    classes = iota((CLASSES, count), 0)
    hot = classes == label
    support = jnp.where(hot & live & jnp.logical_not(odd), 1.0, 0.0)
    counts = jnp.maximum(jnp.sum(support, axis=1, keepdims=True), 1.0)
    support = support.astype(BF16)
    protos = dot(support, embeds, 1, 0) / counts
    parts = three_parts(protos)
    crosses = dot(jnp.concatenate(parts, axis=0), embeds, 1, 1)
    cross = crosses[:CLASSES] + crosses[CLASSES : 2 * CLASSES] + crosses[2 * CLASSES :]
    norm_e = to_lanes(jnp.sum(wide * wide, axis=1, keepdims=True))
    norm_p = jnp.sum(protos * protos, axis=1, keepdims=True)
    distance = norm_e - 2.0 * cross + norm_p
    scores = -distance * D ** (-0.5)
    masked = jnp.where(classes < ways, scores, -1e30)
    top = jnp.max(masked, axis=0, keepdims=True)
    powers = jnp.exp(masked - top)
    total = jnp.sum(powers, axis=0, keepdims=True)
    picked = jnp.sum(jnp.where(hot, scores, 0.0), axis=0, keepdims=True)
    per_query = jnp.where(query > 0.0, top + jnp.log(total) - picked, 0.0)
    queries = jnp.maximum(jnp.sum(query, axis=1, keepdims=True), 1.0)
    loss = jnp.sum(per_query, axis=1, keepdims=True) / queries
    share = query / queries
    by_dist = (jnp.where(hot, 1.0, 0.0) - powers / total) * (share * D ** (-0.5))
    by_parts = three_parts(by_dist)
    pulls = dot(jnp.concatenate(by_parts, axis=0), embeds, 1, 0)
    pull = pulls[:CLASSES] + pulls[CLASSES : 2 * CLASSES] + pulls[2 * CLASSES :]
    by_sums = 2.0 * (protos * jnp.sum(by_dist, axis=1, keepdims=True) - pull) / counts
    sum_parts = three_parts(by_sums)
    left = jnp.concatenate([by_parts[0], by_parts[0], by_parts[1], support, support], axis=0)
    right = jnp.concatenate(
        [-2.0 * parts[0], -2.0 * parts[1], -2.0 * parts[0], sum_parts[0], sum_parts[1]], axis=0
    )
    own = to_sublanes(jnp.sum(by_dist, axis=0, keepdims=True))
    grads = dot(left, right, 0, 0) + 2.0 * own * wide
    return grads.astype(BF16), loss


def kernel(
    n,
    n_group,
    owner_ref,
    slot_ref,
    query_ref,
    ways_ref,
    features_ref,
    weight_hbm,
    out_rows_ref,
    out_weight_ref,
    out_loss_ref,
    weight_ref,
    rows_send,
    rows_recv,
    back_send,
    back_recv,
    halves,
    fold_send,
    fold_recv,
    part_send,
    part_recv,
    cross_send,
    cross_recv,
    whole,
    load_sem,
    rows_ss,
    rows_rs,
    back_ss,
    back_rs,
    fold_ss,
    fold_rs,
    part_ss,
    part_rs,
    cross_ss,
    cross_rs,
    whole_ss,
    whole_rs,
    twin_ss,
    twin_rs,
):
    me = lax.axis_index("dp")
    group = lax.axis_index("group")
    chips = n // 2
    core = lax.rem(me, 2)
    chip = lax.div(me, 2)
    twin = me + 1 - 2 * core
    rows = features_ref.shape[0]
    half = D // 2

    barrier = pltpu.get_barrier_semaphore()

    def greet(step, carry):
        peer = lax.rem(me + step, n)
        pl.semaphore_signal(barrier, inc=1, device_id=(peer, group), device_id_type=MESH)
        return carry

    def greet_group(step, carry):
        peer = lax.rem(group + step, n_group)
        pl.semaphore_signal(barrier, inc=1, device_id=(me, peer), device_id_type=MESH)
        return carry

    lax.fori_loop(1, n, greet, 0)
    lax.fori_loop(1, n_group, greet_group, 0)
    load = pltpu.make_async_copy(weight_hbm, weight_ref, load_sem)
    load.start()

    owner = owner_ref[...].astype(F32)
    owner_lane = to_lanes(owner)
    earlier = (owner == owner_lane) & (iota((rows, rows), 0) < iota((rows, rows), 1))
    place = jnp.sum(jnp.where(earlier, 1.0, 0.0), axis=0, keepdims=True)
    slot = (owner_lane * CAP + place).astype(I32)
    hot = iota((n * CAP, rows), 0) == slot
    codes = (slot_ref[...] * 2 + query_ref[...] + 1).astype(F32)
    code_column = jnp.sum(jnp.where(hot, codes, 0.0), axis=1, keepdims=True)
    hot = jnp.where(hot, 1.0, 0.0).astype(BF16)
    packed = dot(hot, features_ref[...], 1, 0).astype(BF16)
    code_tile = jnp.broadcast_to(code_column, (n * CAP, LANES)).astype(BF16)
    rows_send[...] = jnp.concatenate([packed, code_tile], axis=1).reshape(rows_send.shape)
    rows_recv[me] = rows_send[me]

    pl.semaphore_wait(barrier, n + n_group - 2)

    def send_rows(step, carry):
        peer = lax.rem(me + step, n)
        pltpu.make_async_remote_copy(
            src_ref=rows_send.at[peer],
            dst_ref=rows_recv.at[me],
            send_sem=rows_ss,
            recv_sem=rows_rs,
            device_id=(peer, group),
            device_id_type=MESH,
        ).start()
        return carry

    lax.fori_loop(1, n, send_rows, 0)
    load.wait()
    others = rows_recv.at[pl.ds(0, n - 1)]
    pltpu.make_async_copy(others, others, rows_rs).wait()

    got = rows_recv[...].reshape(n * CAP, D + LANES)
    got_rows = got[:, :D]
    first = jnp.where(iota((8, LANES), 1) == 0, 1.0, 0.0).astype(BF16)
    got_codes = dot(first, got[:, D:], 1, 1)[:1]
    grads, loss = episode(got_rows, got_codes, ways_ref[0], weight_ref[...])
    out_loss_ref[...] = loss

    for part in range(2):
        halves[part] = got_rows[:, part * half : (part + 1) * half]

    def term(which):
        value = dot(halves[which], grads, 0, 0)
        return jnp.concatenate(
            [value[:, i * LANES : (i + 1) * LANES] for i in range(D // LANES)], axis=0
        )

    fold_send[...] = term(1 - core).astype(BF16)
    fold = pltpu.make_async_remote_copy(
        src_ref=fold_send,
        dst_ref=fold_recv,
        send_sem=fold_ss,
        recv_sem=fold_rs,
        device_id=(twin, group),
        device_id_type=MESH,
    )
    fold.start()
    own = term(core)
    outgoing = dot(grads, weight_ref[...], 1, 1).astype(BF16)
    back_send[...] = outgoing.reshape(back_send.shape)
    back_recv[me] = back_send[me]
    fold.wait_recv()
    part_send[...] = (own + fold_recv[...].astype(F32)).astype(BF16).reshape(part_send.shape)
    part_recv[chip] = part_send[chip]

    def send_part(step, carry):
        peer = lax.rem(chip + step, chips)
        pltpu.make_async_remote_copy(
            src_ref=part_send.at[peer],
            dst_ref=part_recv.at[chip],
            send_sem=part_ss,
            recv_sem=part_rs,
            device_id=(2 * peer + core, group),
            device_id_type=MESH,
        ).start()
        return carry

    def send_back(step, carry):
        peer = lax.rem(me + step, n)
        pltpu.make_async_remote_copy(
            src_ref=back_send.at[peer],
            dst_ref=back_recv.at[me],
            send_sem=back_ss,
            recv_sem=back_rs,
            device_id=(peer, group),
            device_id_type=MESH,
        ).start()
        return carry

    lax.fori_loop(1, chips, send_part, 0)
    lax.fori_loop(1, n, send_back, 0)
    others = part_recv.at[pl.ds(0, chips - 1)]
    pltpu.make_async_copy(others, others, part_rs).wait()
    cross_send[...] = jnp.sum(part_recv[...].astype(F32), axis=0)
    cross_recv[group] = cross_send[...]

    def send_cross(step, carry):
        peer = lax.rem(group + step, n_group)
        pltpu.make_async_remote_copy(
            src_ref=cross_send,
            dst_ref=cross_recv.at[group],
            send_sem=cross_ss,
            recv_sem=cross_rs,
            device_id=(me, peer),
            device_id_type=MESH,
        ).start()
        return carry

    lax.fori_loop(1, n_group, send_cross, 0)
    others = cross_recv.at[pl.ds(0, n_group - 1)]
    pltpu.make_async_copy(others, others, cross_rs).wait()
    whole[core, chip] = jnp.sum(cross_recv[...], axis=0).astype(BF16)

    def send_whole(step, carry):
        peer = lax.rem(chip + step, chips)
        pltpu.make_async_remote_copy(
            src_ref=whole.at[core, chip],
            dst_ref=whole.at[core, chip],
            send_sem=whole_ss,
            recv_sem=whole_rs,
            device_id=(2 * peer + core, group),
            device_id_type=MESH,
        ).start()
        return carry

    lax.fori_loop(1, chips, send_whole, 0)

    others = back_recv.at[pl.ds(0, n - 1)]
    pltpu.make_async_copy(others, others, back_rs).wait()
    returned = back_recv[...].reshape(n * CAP, D)
    out_rows_ref[...] = dot(hot, returned, 0, 0).astype(BF16)

    others = whole.at[0, pl.ds(0, chips - 1)]
    pltpu.make_async_copy(others, others, whole_rs).wait()
    last = pltpu.make_async_remote_copy(
        src_ref=whole.at[core],
        dst_ref=whole.at[core],
        send_sem=twin_ss,
        recv_sem=twin_rs,
        device_id=(twin, group),
        device_id_type=MESH,
    )
    last.start()
    sent = rows_send.at[pl.ds(0, n - 1)]
    pltpu.make_async_copy(sent, sent, rows_ss).wait()
    sent = back_send.at[pl.ds(0, n - 1)]
    pltpu.make_async_copy(sent, sent, back_ss).wait()
    sent = part_send.at[pl.ds(0, chips - 1)]
    pltpu.make_async_copy(sent, sent, part_ss).wait()
    sent = whole.at[0, pl.ds(0, chips - 1)]
    pltpu.make_async_copy(sent, sent, whole_ss).wait()
    sent = cross_recv.at[pl.ds(0, n_group - 1)]
    pltpu.make_async_copy(sent, sent, cross_ss).wait()
    fold.wait_send()
    last.wait()
    out_weight_ref[...] = whole[...]


def on_device(n, n_group, features, weight, owner, slots, queries, ways):
    rows = features.shape[0]
    chips = n // 2
    lines = D * D // 2 // LANES
    vmem = pl.BlockSpec(memory_space=pltpu.VMEM)
    dma = pltpu.SemaphoreType.DMA
    part = (chips, lines // chips, LANES)
    own_rows, terms, losses = pl.pallas_call(
        functools.partial(kernel, n, n_group),
        out_shape=(
            jax.ShapeDtypeStruct((rows, D), BF16),
            jax.ShapeDtypeStruct((2, *part), BF16),
            jax.ShapeDtypeStruct((1, 1), F32),
        ),
        in_specs=[
            vmem,
            vmem,
            vmem,
            pl.BlockSpec(memory_space=pltpu.SMEM),
            vmem,
            pl.BlockSpec(memory_space=pl.ANY),
        ],
        out_specs=(vmem, vmem, vmem),
        scratch_shapes=[
            pltpu.VMEM((D, D), BF16),
            pltpu.VMEM((n, CAP, D + LANES), BF16),
            pltpu.VMEM((n, CAP, D + LANES), BF16),
            pltpu.VMEM((n, CAP, D), BF16),
            pltpu.VMEM((n, CAP, D), BF16),
            pltpu.VMEM((2, n * CAP, D // 2), BF16),
            pltpu.VMEM((lines, LANES), BF16),
            pltpu.VMEM((lines, LANES), BF16),
            pltpu.VMEM(part, BF16),
            pltpu.VMEM(part, BF16),
            pltpu.VMEM(part[1:], F32),
            pltpu.VMEM((n_group, *part[1:]), F32),
            pltpu.VMEM((2, *part), BF16),
        ]
        + [dma] * 15,
        compiler_params=pltpu.CompilerParams(collective_id=0, has_side_effects=True),
        name="episodes",
    )(owner, slots.reshape(1, rows), queries.reshape(1, rows), ways, features, weight)
    blocks = terms.reshape(2, D // LANES, D // 2, LANES)
    grad_weight = jnp.swapaxes(blocks, 1, 2).reshape(D, D).astype(F32)
    return own_rows, grad_weight, losses.reshape(1)


def solution(mesh):
    both = P(("dp", "group"))
    lines = P(("dp", "group"), None)
    return jax.shard_map(
        functools.partial(on_device, mesh.shape["dp"], mesh.shape["group"]),
        mesh=mesh,
        in_specs=(lines, P(), lines, both, both, both),
        out_specs=(lines, P(), both),
        check_vma=False,
    )
```

```python
import functools
import math

import jax
import jax.numpy as jnp
from jax import lax
from jax.experimental import pallas as pl
from jax.experimental.pallas import tpu as pltpu
from jax.sharding import PartitionSpec as P

D = 512
WAYS_MAX = 50
CLASSES = 64
CAP = 2
LANES = 128
MESH = pl.DeviceIdType.MESH
F32 = jnp.float32
BF16 = jnp.bfloat16
I32 = jnp.int32
BACK = (0, 0)


def dot(a, b, ca, cb):
    return lax.dot_general(a, b, (((ca,), (cb,)), ((), ())), preferred_element_type=F32)


def iota(shape, dim):
    return lax.broadcasted_iota(I32, shape, dim)


def three_parts(x):
    hi = x.astype(BF16)
    rest = x - hi.astype(F32)
    mid = rest.astype(BF16)
    low = (rest - mid.astype(F32)).astype(BF16)
    return hi, mid, low


def to_lanes(column):
    n = column.shape[0]
    same = iota((n, n), 0) == iota((n, n), 1)
    return jnp.sum(jnp.where(same, column, 0.0), axis=0, keepdims=True)


def to_sublanes(row):
    n = row.shape[1]
    same = iota((n, n), 0) == iota((n, n), 1)
    return jnp.sum(jnp.where(same, row, 0.0), axis=1, keepdims=True)


def episode(rows, codes, ways, weight):
    count = rows.shape[0]
    embeds = dot(rows, weight, 1, 0).astype(BF16)
    wide = embeds.astype(F32)
    code = codes.astype(I32)
    value = jnp.maximum(code - 1, 0)
    live = code > 0
    odd = lax.rem(value, 2) == 1
    query = (live & odd).astype(F32)
    label = lax.div(value, 2)
    for factor in (8, 4, 2, 1):
        label = jnp.where(label >= factor * ways, label - factor * ways, label)
    classes = iota((CLASSES, count), 0)
    hot = classes == label
    support = jnp.where(hot & live & jnp.logical_not(odd), 1.0, 0.0)
    counts = jnp.maximum(jnp.sum(support, axis=1, keepdims=True), 1.0)
    support = support.astype(BF16)
    protos = dot(support, embeds, 1, 0) / counts
    parts = three_parts(protos)
    crosses = dot(jnp.concatenate(parts, axis=0), embeds, 1, 1)
    cross = crosses[:CLASSES] + crosses[CLASSES : 2 * CLASSES] + crosses[2 * CLASSES :]
    norm_e = to_lanes(jnp.sum(wide * wide, axis=1, keepdims=True))
    norm_p = jnp.sum(protos * protos, axis=1, keepdims=True)
    distance = norm_e - 2.0 * cross + norm_p
    scores = -distance * D ** (-0.5)
    masked = jnp.where(classes < ways, scores, -1e30)
    top = jnp.max(masked, axis=0, keepdims=True)
    powers = jnp.exp(masked - top)
    total = jnp.sum(powers, axis=0, keepdims=True)
    picked = jnp.sum(jnp.where(hot, scores, 0.0), axis=0, keepdims=True)
    per_query = jnp.where(query > 0.0, top + jnp.log(total) - picked, 0.0)
    queries = jnp.maximum(jnp.sum(query, axis=1, keepdims=True), 1.0)
    loss = jnp.sum(per_query, axis=1, keepdims=True) / queries
    share = query / queries
    by_dist = (jnp.where(hot, 1.0, 0.0) - powers / total) * (share * D ** (-0.5))
    by_parts = three_parts(by_dist)
    pulls = dot(jnp.concatenate(by_parts, axis=0), embeds, 1, 0)
    pull = pulls[:CLASSES] + pulls[CLASSES : 2 * CLASSES] + pulls[2 * CLASSES :]
    by_sums = 2.0 * (protos * jnp.sum(by_dist, axis=1, keepdims=True) - pull) / counts
    sum_parts = three_parts(by_sums)
    left = jnp.concatenate([by_parts[0], by_parts[0], by_parts[1], support, support], axis=0)
    right = jnp.concatenate(
        [-2.0 * parts[0], -2.0 * parts[1], -2.0 * parts[0], sum_parts[0], sum_parts[1]], axis=0
    )
    own = to_sublanes(jnp.sum(by_dist, axis=0, keepdims=True))
    grads = dot(left, right, 0, 0) + 2.0 * own * wide
    return grads.astype(BF16), loss


def farthest_first(count):
    return sorted(range(count), key=lambda i: -min(i, count - i))


def arrived(block, sem):
    pltpu.make_async_copy(block, block, sem).wait()


def lay_out(blocks, out_ref, which):
    lines = out_ref.shape[0] // 2
    value = blocks[which].reshape(D // LANES, lines, LANES)
    start = pl.multiple_of(which * lines, lines)
    for i in range(D // LANES):
        out_ref[pl.ds(start, lines), i * LANES : (i + 1) * LANES] = value[i].astype(F32)


def kernel(
    n,
    n_group,
    owner_hbm,
    slot_hbm,
    query_hbm,
    ways_hbm,
    features_hbm,
    weight_hbm,
    out_rows_ref,
    out_weight_ref,
    out_loss_ref,
    owner_ref,
    slot_ref,
    query_ref,
    ways_ref,
    features_ref,
    weight_ref,
    rows_send,
    rows_recv,
    back_send,
    back_recv,
    halves,
    fold_send,
    fold_recv,
    part_send,
    part_recv,
    line_send,
    line_recv,
    cross_send,
    cross_recv,
    whole,
    load_sem,
    rows_ss,
    rows_rs,
    back_ss,
    back_rs,
    fold_ss,
    fold_rs,
    part_ss,
    part_rs,
    line_ss,
    line_rs,
    cross_ss,
    cross_rs,
    whole_ss,
    whole_rs,
    twin_ss,
    twin_rs,
):
    me = lax.axis_index("dp")
    group = lax.axis_index("group")
    chips = n // 2
    side = math.isqrt(chips)
    core = lax.rem(me, 2)
    chip = lax.div(me, 2)
    high = lax.div(chip, side)
    low = lax.rem(chip, side)
    twin = me + 1 - 2 * core
    rows = features_ref.shape[0]
    half = D // 2
    offsets = farthest_first(side)
    highs = [lax.rem(high + i, side) * (2 * side) for i in range(side)]
    lows = [lax.rem(low + i, side) * 2 for i in range(side)]
    groups = [lax.rem(group + i, n_group) for i in range(1, n_group)]
    plane = [(h, w) for h in offsets for w in offsets if h or w]
    row_peers = [highs[h] + lows[w] + c for h, w in plane for c in range(2)] + [twin]
    lines = [
        (low, [(lax.rem(low + i, side), highs[0] + lows[i] + core) for i in offsets if i]),
        (high, [(lax.rem(high + i, side), highs[i] + lows[0] + core) for i in offsets if i]),
    ]

    barrier = pltpu.get_barrier_semaphore()
    with jax.named_scope("greet"):
        for peer in row_peers:
            pl.semaphore_signal(barrier, inc=1, device_id=(peer, group), device_id_type=MESH)
        for peer in groups:
            pl.semaphore_signal(barrier, inc=1, device_id=(me, peer), device_id_type=MESH)
    loads = [
        pltpu.make_async_copy(source, target, load_sem.at[i])
        for i, (source, target) in enumerate(
            (
                (owner_hbm, owner_ref),
                (features_hbm, features_ref),
                (slot_hbm, slot_ref),
                (query_hbm, query_ref),
                (ways_hbm, ways_ref),
                (weight_hbm, weight_ref),
            )
        )
    ]
    for load in loads:
        load.start()
    for load in loads:
        load.wait()

    owner_lane = owner_ref[...].astype(F32)
    owner = to_sublanes(owner_lane)
    earlier = (owner == owner_lane) & (iota((rows, rows), 0) < iota((rows, rows), 1))
    place = jnp.sum(jnp.where(earlier, 1.0, 0.0), axis=0, keepdims=True)
    slot = (owner_lane * CAP + place).astype(I32)
    hot = iota((n * CAP, rows), 0) == slot
    codes = (slot_ref[...] * 2 + query_ref[...] + 1).astype(F32)
    code_column = jnp.sum(jnp.where(hot, codes, 0.0), axis=1, keepdims=True)
    hot = jnp.where(hot, 1.0, 0.0).astype(BF16)
    packed = dot(hot, features_ref[...], 1, 0).astype(BF16)
    code_tile = jnp.broadcast_to(code_column, (n * CAP, LANES)).astype(BF16)
    rows_send[...] = jnp.concatenate([packed, code_tile], axis=1).reshape(rows_send.shape)
    rows_recv[me] = rows_send[me]

    with jax.named_scope("barrier_wait"):
        pl.semaphore_wait(barrier, n + n_group - 2)

    with jax.named_scope("send_rows"):
        for peer in row_peers:
            pltpu.make_async_remote_copy(
                src_ref=rows_send.at[peer],
                dst_ref=rows_recv.at[me],
                send_sem=rows_ss,
                recv_sem=rows_rs,
                device_id=(peer, group),
                device_id_type=MESH,
            ).start()
    others = rows_recv.at[pl.ds(0, n - 1)]
    with jax.named_scope("rows_wait"):
        pltpu.make_async_copy(others, others, rows_rs).wait()

    got = rows_recv[...].reshape(n * CAP, D + LANES)
    got_rows = got[:, :D]
    first = jnp.where(iota((8, LANES), 1) == 0, 1.0, 0.0).astype(BF16)
    got_codes = dot(first, got[:, D:], 1, 1)[:1]
    with jax.named_scope("episode"):
        grads, loss = episode(got_rows, got_codes, ways_ref[...], weight_ref[...])
        out_loss_ref[...] = loss

    for part in range(2):
        halves[part] = got_rows[:, part * half : (part + 1) * half]

    def term(which):
        value = dot(halves[which], grads, 0, 0)
        return jnp.concatenate(
            [value[:, i * LANES : (i + 1) * LANES] for i in range(D // LANES)], axis=0
        )

    fold_send[...] = term(1 - core).astype(BF16)
    fold = pltpu.make_async_remote_copy(
        src_ref=fold_send,
        dst_ref=fold_recv,
        send_sem=fold_ss,
        recv_sem=fold_rs,
        device_id=(twin, group),
        device_id_type=MESH,
    )
    fold.start()
    own = term(core)
    outgoing = dot(grads, weight_ref[...], 1, 1).astype(BF16)
    back_send[...] = outgoing.reshape(back_send.shape)
    back_recv[me] = back_send[me]
    with jax.named_scope("fold_wait"):
        fold.wait_recv()
    part_send[...] = (own + fold_recv[...].astype(F32)).astype(BF16).reshape(part_send.shape)

    def along(axis, source, target, send_sem, recv_sem):
        for place, peer in lines[axis][1]:
            pltpu.make_async_remote_copy(
                src_ref=source(place),
                dst_ref=target,
                send_sem=send_sem,
                recv_sem=recv_sem,
                device_id=(peer, group),
                device_id_type=MESH,
            ).start()

    def send_back(peers):
        with jax.named_scope("send_back"):
            for peer in peers:
                pltpu.make_async_remote_copy(
                    src_ref=back_send.at[peer],
                    dst_ref=back_recv.at[me],
                    send_sem=back_ss,
                    recv_sem=back_rs,
                    device_id=(peer, group),
                    device_id_type=MESH,
                ).start()

    for i in range(2):
        here = lines[i][0]
        along(i, lambda p: part_send.at[i, p], part_recv.at[i, here], part_ss.at[i], part_rs.at[i])
        part_recv[i, here] = part_send[i, here]
    send_back(row_peers[: BACK[0]])
    for i in range(2):
        with jax.named_scope(f"part_wait{i}"):
            arrived(part_recv.at[i, pl.ds(0, side - 1)], part_rs.at[i])
        line_send[i] = jnp.sum(part_recv[i].astype(F32), axis=0).astype(BF16)
        here = lines[1 - i][0]
        along(1 - i, lambda p: line_send.at[i], line_recv.at[i, here], line_ss.at[i], line_rs.at[i])
        line_recv[i, here] = line_send[i]
    send_back(row_peers[BACK[0] : BACK[1]])
    for i in range(2):
        with jax.named_scope(f"line_wait{i}"):
            arrived(line_recv.at[i, pl.ds(0, side - 1)], line_rs.at[i])
        cross_send[i] = jnp.sum(line_recv[i].astype(F32), axis=0).astype(BF16)
        for peer in groups:
            pltpu.make_async_remote_copy(
                src_ref=cross_send.at[i],
                dst_ref=cross_recv.at[i, group],
                send_sem=cross_ss.at[i],
                recv_sem=cross_rs.at[i],
                device_id=(me, peer),
                device_id_type=MESH,
            ).start()
        cross_recv[i, group] = cross_send[i]
    send_back(row_peers[BACK[1] :])
    for i in range(2):
        with jax.named_scope(f"cross_wait{i}"):
            arrived(cross_recv.at[i, pl.ds(0, n_group - 1)], cross_rs.at[i])
        here = lines[i][0]
        whole[core, i, here] = jnp.sum(cross_recv[i].astype(F32), axis=0).astype(BF16)
        final = whole.at[core, i, here]
        along(i, lambda p: final, final, whole_ss.at[i], whole_rs.at[i])

    others = back_recv.at[pl.ds(0, n - 1)]
    with jax.named_scope("back_wait"):
        pltpu.make_async_copy(others, others, back_rs).wait()
    returned = back_recv[...].reshape(n * CAP, D)
    out_rows_ref[...] = dot(hot, returned, 0, 0).astype(BF16)

    with jax.named_scope("whole_wait"):
        for i in range(2):
            arrived(whole.at[0, i, pl.ds(0, side - 1)], whole_rs.at[i])
    last = pltpu.make_async_remote_copy(
        src_ref=whole.at[core],
        dst_ref=whole.at[core],
        send_sem=twin_ss,
        recv_sem=twin_rs,
        device_id=(twin, group),
        device_id_type=MESH,
    )
    last.start()
    lay_out(whole, out_weight_ref, core)
    sent = rows_send.at[pl.ds(0, n - 1)]
    pltpu.make_async_copy(sent, sent, rows_ss).wait()
    sent = back_send.at[pl.ds(0, n - 1)]
    pltpu.make_async_copy(sent, sent, back_ss).wait()
    for i in range(2):
        arrived(part_recv.at[i, pl.ds(0, side - 1)], part_ss.at[i])
        arrived(line_recv.at[i, pl.ds(0, side - 1)], line_ss.at[i])
        arrived(cross_recv.at[i, pl.ds(0, n_group - 1)], cross_ss.at[i])
        arrived(part_recv.at[i, pl.ds(0, side - 1)], whole_ss.at[i])
    fold.wait_send()
    with jax.named_scope("last_wait"):
        last.wait()
    lay_out(whole, out_weight_ref, 1 - core)


def put_out(rows_ref, terms_ref, loss_ref, out_rows, out_terms, out_loss, sems):
    pairs = ((terms_ref, out_terms), (rows_ref, out_rows), (loss_ref, out_loss))
    copies = [pltpu.make_async_copy(a, b, sems.at[i]) for i, (a, b) in enumerate(pairs)]
    for copy in copies:
        copy.start()
    for copy in copies:
        copy.wait()


def on_device(n, n_group, features, weight, owner, slots, queries, ways):
    rows = features.shape[0]
    chips = n // 2
    lines = D * D // 2 // LANES
    vmem = pl.BlockSpec(memory_space=pltpu.VMEM)
    dma = pltpu.SemaphoreType.DMA
    side = math.isqrt(chips)
    part = (2, side, lines // (2 * side), LANES)
    hbm = pl.BlockSpec(memory_space=pl.ANY)
    own_rows, terms, losses = pl.pallas_call(
        functools.partial(kernel, n, n_group),
        out_shape=(
            pltpu.VMEM((rows, D), BF16),
            pltpu.VMEM((D, D), F32),
            pltpu.VMEM((1, 1), F32),
        ),
        in_specs=[hbm] * 6,
        out_specs=(vmem, vmem, vmem),
        scratch_shapes=[
            pltpu.VMEM((1, rows), I32),
            pltpu.VMEM((1, rows), I32),
            pltpu.VMEM((1, rows), I32),
            pltpu.VMEM((1, 1), I32),
            pltpu.VMEM((rows, D), BF16),
            pltpu.VMEM((D, D), BF16),
            pltpu.VMEM((n, CAP, D + LANES), BF16),
            pltpu.VMEM((n, CAP, D + LANES), BF16),
            pltpu.VMEM((n, CAP, D), BF16),
            pltpu.VMEM((n, CAP, D), BF16),
            pltpu.VMEM((2, n * CAP, D // 2), BF16),
            pltpu.VMEM((lines, LANES), BF16),
            pltpu.VMEM((lines, LANES), BF16),
            pltpu.VMEM(part, BF16),
            pltpu.VMEM(part, BF16),
            pltpu.VMEM((2, *part[2:]), BF16),
            pltpu.VMEM(part, BF16),
            pltpu.VMEM((2, *part[2:]), BF16),
            pltpu.VMEM((2, n_group, *part[2:]), BF16),
            pltpu.VMEM((2, *part), BF16),
            pltpu.SemaphoreType.DMA((6,)),
        ]
        + [dma] * 6
        + [pltpu.SemaphoreType.DMA((2,))] * 8
        + [dma] * 2,
        compiler_params=pltpu.CompilerParams(collective_id=0, has_side_effects=True),
        name="episodes",
    )(
        owner.reshape(1, rows),
        slots.reshape(1, rows),
        queries.reshape(1, rows),
        ways.reshape(1, 1),
        features,
        weight,
    )
    own_rows, terms, losses = pl.pallas_call(
        put_out,
        out_shape=(
            jax.ShapeDtypeStruct((rows, D), BF16),
            jax.ShapeDtypeStruct((D, D), F32),
            jax.ShapeDtypeStruct((1, 1), F32),
        ),
        in_specs=[vmem] * 3,
        out_specs=(hbm, hbm, hbm),
        scratch_shapes=[pltpu.SemaphoreType.DMA((3,))],
        name="results",
    )(*(pltpu.with_memory_space_constraint(x, pltpu.VMEM) for x in (own_rows, terms, losses)))
    return own_rows, terms, losses.reshape(1)


def solution(mesh):
    both = P(("dp", "group"))
    lines = P(("dp", "group"), None)
    return jax.shard_map(
        functools.partial(on_device, mesh.shape["dp"], mesh.shape["group"]),
        mesh=mesh,
        in_specs=(lines, P(), lines, both, both, both),
        out_specs=(lines, P(), both),
        check_vma=False,
    )
```

```python
import functools
import math

import jax
import jax.numpy as jnp
from jax import lax
from jax.experimental import pallas as pl
from jax.experimental.pallas import tpu as pltpu
from jax.sharding import PartitionSpec as P

D = 512
WAYS_MAX = 50
CLASSES = 64
CAP = 2
LANES = 128
MESH = pl.DeviceIdType.MESH
F32 = jnp.float32
BF16 = jnp.bfloat16
I32 = jnp.int32
BACK = ((0, 0, 127), (0, 127, 127))


def dot(a, b, ca, cb):
    return lax.dot_general(a, b, (((ca,), (cb,)), ((), ())), preferred_element_type=F32)


def iota(shape, dim):
    return lax.broadcasted_iota(I32, shape, dim)


def three_parts(x):
    hi = x.astype(BF16)
    rest = x - hi.astype(F32)
    mid = rest.astype(BF16)
    low = (rest - mid.astype(F32)).astype(BF16)
    return hi, mid, low


def to_lanes(column):
    n = column.shape[0]
    same = iota((n, n), 0) == iota((n, n), 1)
    return jnp.sum(jnp.where(same, column, 0.0), axis=0, keepdims=True)


def to_sublanes(row):
    n = row.shape[1]
    same = iota((n, n), 0) == iota((n, n), 1)
    return jnp.sum(jnp.where(same, row, 0.0), axis=1, keepdims=True)


def episode(rows, codes, ways, weight):
    count = rows.shape[0]
    embeds = dot(rows, weight, 1, 0).astype(BF16)
    wide = embeds.astype(F32)
    code = codes.astype(I32)
    value = jnp.maximum(code - 1, 0)
    live = code > 0
    odd = lax.rem(value, 2) == 1
    query = (live & odd).astype(F32)
    label = lax.div(value, 2)
    for factor in (8, 4, 2, 1):
        label = jnp.where(label >= factor * ways, label - factor * ways, label)
    classes = iota((CLASSES, count), 0)
    hot = classes == label
    support = jnp.where(hot & live & jnp.logical_not(odd), 1.0, 0.0)
    counts = jnp.maximum(jnp.sum(support, axis=1, keepdims=True), 1.0)
    support = support.astype(BF16)
    protos = dot(support, embeds, 1, 0) / counts
    parts = three_parts(protos)
    crosses = dot(jnp.concatenate(parts, axis=0), embeds, 1, 1)
    cross = crosses[:CLASSES] + crosses[CLASSES : 2 * CLASSES] + crosses[2 * CLASSES :]
    norm_e = to_lanes(jnp.sum(wide * wide, axis=1, keepdims=True))
    norm_p = jnp.sum(protos * protos, axis=1, keepdims=True)
    distance = norm_e - 2.0 * cross + norm_p
    scores = -distance * D ** (-0.5)
    masked = jnp.where(classes < ways, scores, -1e30)
    top = jnp.max(masked, axis=0, keepdims=True)
    powers = jnp.exp(masked - top)
    total = jnp.sum(powers, axis=0, keepdims=True)
    picked = jnp.sum(jnp.where(hot, scores, 0.0), axis=0, keepdims=True)
    per_query = jnp.where(query > 0.0, top + jnp.log(total) - picked, 0.0)
    queries = jnp.maximum(jnp.sum(query, axis=1, keepdims=True), 1.0)
    loss = jnp.sum(per_query, axis=1, keepdims=True) / queries
    share = query / queries
    by_dist = (jnp.where(hot, 1.0, 0.0) - powers / total) * (share * D ** (-0.5))
    by_parts = three_parts(by_dist)
    pulls = dot(jnp.concatenate(by_parts, axis=0), embeds, 1, 0)
    pull = pulls[:CLASSES] + pulls[CLASSES : 2 * CLASSES] + pulls[2 * CLASSES :]
    by_sums = 2.0 * (protos * jnp.sum(by_dist, axis=1, keepdims=True) - pull) / counts
    sum_parts = three_parts(by_sums)
    left = jnp.concatenate([by_parts[0], by_parts[0], by_parts[1], support, support], axis=0)
    right = jnp.concatenate(
        [-2.0 * parts[0], -2.0 * parts[1], -2.0 * parts[0], sum_parts[0], sum_parts[1]], axis=0
    )
    own = to_sublanes(jnp.sum(by_dist, axis=0, keepdims=True))
    grads = dot(left, right, 0, 0) + 2.0 * own * wide
    return grads.astype(BF16), loss


def farthest_first(count):
    return sorted(range(count), key=lambda i: -min(i, count - i))


def one_hot(places, count):
    return jnp.where(iota((count, places.shape[1]), 0) == places, 1.0, 0.0).astype(BF16)


def arrived(block, sem):
    pltpu.make_async_copy(block, block, sem).wait()


def lay_out(blocks, out_ref, which):
    lines = out_ref.shape[0] // 2
    value = blocks[which].reshape(D // LANES, lines, LANES)
    start = which * lines
    for i in range(D // LANES):
        out_ref[start : start + lines, i * LANES : (i + 1) * LANES] = value[i].astype(F32)


def kernel(
    n,
    n_group,
    owner_hbm,
    slot_hbm,
    query_hbm,
    ways_hbm,
    features_hbm,
    weight_hbm,
    out_rows_ref,
    out_weight_ref,
    out_loss_ref,
    owner_ref,
    slot_ref,
    query_ref,
    ways_ref,
    features_ref,
    weight_ref,
    code_send,
    code_mid,
    code_recv,
    left_send,
    left_mid,
    left_recv,
    right_send,
    right_mid,
    right_recv,
    back_send,
    back_recv,
    halves,
    fold_send,
    fold_recv,
    part_send,
    part_recv,
    line_send,
    line_recv,
    cross_send,
    cross_recv,
    whole,
    load_sem,
    code_ss,
    code_rs,
    left_ss,
    left_rs,
    right_ss,
    right_rs,
    back_ss,
    back_rs,
    fold_ss,
    fold_rs,
    part_ss,
    part_rs,
    line_ss,
    line_rs,
    cross_ss,
    cross_rs,
    whole_ss,
    whole_rs,
    twin_ss,
    twin_rs,
    tick,
):
    me = lax.axis_index("dp")
    group = lax.axis_index("group")
    chips = n // 2
    side = math.isqrt(chips)
    core = lax.rem(me, 2)
    chip = lax.div(me, 2)
    high = lax.div(chip, side)
    low = lax.rem(chip, side)
    twin = me + 1 - 2 * core
    rows = features_ref.shape[0]
    half = D // 2
    offsets = farthest_first(side)
    highs = [lax.rem(high + i, side) * (2 * side) for i in range(side)]
    lows = [lax.rem(low + i, side) * 2 for i in range(side)]
    wide = 2 * side
    mine = 2 * low + core
    row_line = [(2 * lax.rem(low + i, side) + c, highs[0] + lows[i] + c) for i in offsets if i for c in range(2)]
    row_line.append((mine + 1 - 2 * core, twin))
    groups = [lax.rem(group + i, n_group) for i in range(1, n_group)]
    plane = [(h, w) for h in offsets for w in offsets if h or w]
    row_peers = [highs[h] + lows[w] + c for h, w in plane for c in range(2)] + [twin]
    lines = [
        (low, [(lax.rem(low + i, side), highs[0] + lows[i] + core) for i in offsets if i]),
        (high, [(lax.rem(high + i, side), highs[i] + lows[0] + core) for i in offsets if i]),
    ]

    barrier = pltpu.get_barrier_semaphore()
    with jax.named_scope("greet"):
        for _, peer in row_line + lines[1][1]:
            pl.semaphore_signal(barrier, inc=1, device_id=(peer, group), device_id_type=MESH)
        for peer in groups:
            pl.semaphore_signal(barrier, inc=1, device_id=(me, peer), device_id_type=MESH)
    loads = [
        pltpu.make_async_copy(source, target, load_sem.at[i])
        for i, (source, target) in enumerate(
            (
                (owner_hbm, owner_ref),
                (features_hbm, features_ref),
                (slot_hbm, slot_ref),
                (query_hbm, query_ref),
                (ways_hbm, ways_ref),
                (weight_hbm, weight_ref),
            )
        )
    ]
    for load in loads:
        load.start()
    for load in loads:
        load.wait()

    owner_lane = owner_ref[...].astype(F32)
    owner = to_sublanes(owner_lane)
    earlier = (owner == owner_lane) & (iota((rows, rows), 0) < iota((rows, rows), 1))
    place = jnp.sum(jnp.where(earlier, 1.0, 0.0), axis=0, keepdims=True)
    codes = (slot_ref[...] * 2 + query_ref[...] + 1).astype(F32)
    weighed = to_sublanes(codes * jnp.where(place > 0.0, 1.0 * LANES, 1.0))
    code_send[...] = jnp.sum(
        jnp.where(owner == iota((rows, n), 1).astype(F32), weighed, 0.0), axis=0, keepdims=True
    )
    code_mid[mine] = code_send[...]
    target = owner_lane.astype(I32)
    place = place.astype(I32)
    hot = one_hot(target * CAP + place, n * CAP)
    turned = (lax.rem(target, wide) * side + lax.div(target, wide)) * CAP + place
    left = dot(one_hot(turned, n * CAP), features_ref[:, :half], 1, 0).astype(BF16)
    left_send[...] = left.reshape(left_send.shape)
    right = dot(hot, features_ref[:, half:], 1, 0).astype(BF16)
    right_send[...] = right.reshape(right_send.shape)
    left_mid[:, mine] = left_send[mine]
    right_mid[:, high] = right_send[high]

    with jax.named_scope("barrier_wait"):
        pl.semaphore_wait(barrier, wide + side + n_group - 3)

    def push(source, target, send_sem, recv_sem, peer):
        pltpu.make_async_remote_copy(
            src_ref=source,
            dst_ref=target,
            send_sem=send_sem,
            recv_sem=recv_sem,
            device_id=(peer, group),
            device_id_type=MESH,
        ).start()

    with jax.named_scope("send_rows"):
        for place, peer in row_line:
            push(code_send, code_mid.at[mine], code_ss.at[0], code_rs.at[0], peer)
        for place, peer in row_line:
            push(left_send.at[place], left_mid.at[:, mine], left_ss.at[0], left_rs.at[0], peer)
        for place, peer in lines[1][1]:
            push(right_send.at[place], right_mid.at[:, high], right_ss.at[0], right_rs.at[0], peer)
    with jax.named_scope("code_wait0"):
        arrived(code_mid.at[pl.ds(0, wide - 1)], code_rs.at[0])
    for place, peer in lines[1][1]:
        push(code_mid, code_recv.at[high], code_ss.at[1], code_rs.at[1], peer)
    code_recv[high] = code_mid[...]
    with jax.named_scope("left_wait0"):
        arrived(left_mid.at[:, pl.ds(0, wide - 1)], left_rs.at[0])
    for place, peer in lines[1][1]:
        push(left_mid.at[place], left_recv.at[high], left_ss.at[1], left_rs.at[1], peer)
    left_recv[high] = left_mid[high]
    with jax.named_scope("right_wait0"):
        arrived(right_mid.at[:, pl.ds(0, side - 1)], right_rs.at[0])
    for place, peer in row_line:
        push(right_mid.at[place], right_recv.at[:, mine], right_ss.at[1], right_rs.at[1], peer)
    right_recv[:, mine] = right_mid[mine]
    with jax.named_scope("code_wait1"):
        arrived(code_recv.at[pl.ds(0, side - 1)], code_rs.at[1])
    table = code_recv[...].reshape(n, n)
    both = jnp.sum(jnp.where(iota((n, n), 1) == me, table, 0.0), axis=1, keepdims=True).astype(I32)
    spot = iota((n, n * CAP), 1)
    chosen = jnp.where(lax.rem(spot, CAP) == 0, lax.rem(both, LANES), lax.div(both, LANES))
    chosen = jnp.where(lax.div(spot, CAP) == iota((n, n * CAP), 0), chosen, 0)
    got_codes = jnp.sum(chosen.astype(F32), axis=0, keepdims=True)
    with jax.named_scope("left_wait1"):
        arrived(left_recv.at[pl.ds(0, side - 1)], left_rs.at[1])
    halves[0] = left_recv[...].reshape(n * CAP, half)
    with jax.named_scope("right_wait1"):
        arrived(right_recv.at[:, pl.ds(0, wide - 1)], right_rs.at[1])
    halves[1] = right_recv[...].reshape(n * CAP, half)
    got_rows = jnp.concatenate([halves[0], halves[1]], axis=1)
    with jax.named_scope("episode"):
        grads, loss = episode(got_rows, got_codes, ways_ref[...], weight_ref[...])
        out_loss_ref[...] = loss

    def term(which):
        value = dot(halves[which], grads, 0, 0)
        return jnp.concatenate(
            [value[:, i * LANES : (i + 1) * LANES] for i in range(D // LANES)], axis=0
        )

    def fold(which):
        return pltpu.make_async_remote_copy(
            src_ref=fold_send.at[which],
            dst_ref=fold_recv.at[which],
            send_sem=fold_ss.at[which],
            recv_sem=fold_rs.at[which],
            device_id=(twin, group),
            device_id_type=MESH,
        )

    def last(which):
        return pltpu.make_async_remote_copy(
            src_ref=whole.at[which],
            dst_ref=whole.at[which],
            send_sem=twin_ss.at[which],
            recv_sem=twin_rs.at[which],
            device_id=(twin, group),
            device_id_type=MESH,
        )

    def prepare_back():
        outgoing = dot(grads, weight_ref[...], 1, 1).astype(BF16)
        back_send[...] = outgoing.reshape(back_send.shape)
        back_recv[me] = back_send[me]

    def send_back(which, piece):
        with jax.named_scope(f"send_back{piece}"):
            for peer in row_peers[BACK[which][piece] : BACK[which][piece + 1]]:
                push(back_send.at[peer], back_recv.at[me], back_ss, back_rs, peer)

    def take_back():
        with jax.named_scope("back_wait"):
            arrived(back_recv.at[pl.ds(0, n - 1)], back_rs)
        returned = back_recv[...].reshape(n * CAP, D)
        out_rows_ref[...] = dot(hot, returned, 0, 0).astype(BF16)

    def spread(axis, source, target, send_sem, recv_sem):
        for place, peer in lines[axis][1]:
            push(source(place), target, send_sem, recv_sem, peer)

    def tell():
        pl.semaphore_signal(tick, inc=1, device_id=(twin, group), device_id_type=MESH)

    @pl.when(core == 1)
    def _():
        own = [term(0), term(1)]
        prepare_back()
        for i in range(2):
            with jax.named_scope(f"fold_wait{i}"):
                fold(i).wait_recv()
            total = own[i] + fold_recv[i].astype(F32)
            part_send[i] = total.astype(BF16).reshape(part_send.shape[1:])
            here = lines[i][0]
            spread(i, lambda p: part_send.at[i, p], part_recv.at[i, here], part_ss.at[i], part_rs.at[i])
            part_recv[i, here] = part_send[i, here]
        for i in range(2):
            with jax.named_scope(f"part_wait{i}"):
                arrived(part_recv.at[i, pl.ds(0, side - 1)], part_rs.at[i])
            line_send[i] = jnp.sum(part_recv[i].astype(F32), axis=0).astype(BF16)
            here = lines[1 - i][0]
            spread(1 - i, lambda p: line_send.at[i], line_recv.at[i, here], line_ss.at[i], line_rs.at[i])
            line_recv[i, here] = line_send[i]
        tell()
        send_back(1, 0)
        for i in range(2):
            with jax.named_scope(f"line_wait{i}"):
                arrived(line_recv.at[i, pl.ds(0, side - 1)], line_rs.at[i])
            cross_send[i] = jnp.sum(line_recv[i].astype(F32), axis=0).astype(BF16)
            for peer in groups:
                pltpu.make_async_remote_copy(
                    src_ref=cross_send.at[i],
                    dst_ref=cross_recv.at[i, group],
                    send_sem=cross_ss.at[i],
                    recv_sem=cross_rs.at[i],
                    device_id=(me, peer),
                    device_id_type=MESH,
                ).start()
            cross_recv[i, group] = cross_send[i]
        tell()
        send_back(1, 1)
        for i in range(2):
            with jax.named_scope(f"cross_wait{i}"):
                arrived(cross_recv.at[i, pl.ds(0, n_group - 1)], cross_rs.at[i])
            here = lines[i][0]
            whole[i, here] = jnp.sum(cross_recv[i].astype(F32), axis=0).astype(BF16)
            final = whole.at[i, here]
            spread(i, lambda p: final, final, whole_ss.at[i], whole_rs.at[i])
        for i in range(2):
            with jax.named_scope(f"whole_wait{i}"):
                arrived(whole.at[i, pl.ds(0, side - 1)], whole_rs.at[i])
            last(i).start()
        for i in range(2):
            lay_out(whole, out_weight_ref, i)
        take_back()
        for i in range(2):
            arrived(part_recv.at[i, pl.ds(0, side - 1)], part_ss.at[i])
            arrived(line_recv.at[i, pl.ds(0, side - 1)], line_ss.at[i])
            arrived(cross_recv.at[i, pl.ds(0, n_group - 1)], cross_ss.at[i])
            arrived(part_recv.at[i, pl.ds(0, side - 1)], whole_ss.at[i])
            last(i).wait_send()

    @pl.when(core == 0)
    def _():
        for i in range(2):
            fold_send[i] = term(i).astype(BF16)
            fold(i).start()
        prepare_back()
        for piece in range(2):
            with jax.named_scope(f"tick_wait{piece}"):
                pl.semaphore_wait(tick, 1)
            send_back(0, piece)
        take_back()
        for i in range(2):
            fold(i).wait_send()
            with jax.named_scope(f"last_wait{i}"):
                last(i).wait_recv()
            lay_out(whole, out_weight_ref, i)

    arrived(code_mid.at[pl.ds(0, wide - 1)], code_ss.at[0])
    arrived(code_recv.at[pl.ds(0, side - 1)], code_ss.at[1])
    arrived(left_mid.at[:, pl.ds(0, wide - 1)], left_ss.at[0])
    arrived(left_recv.at[pl.ds(0, side - 1)], left_ss.at[1])
    arrived(right_mid.at[:, pl.ds(0, side - 1)], right_ss.at[0])
    arrived(right_recv.at[:, pl.ds(0, wide - 1)], right_ss.at[1])
    arrived(back_send.at[pl.ds(0, n - 1)], back_ss)


def put_out(rows_ref, terms_ref, loss_ref, out_rows, out_terms, out_loss, sems):
    pairs = ((terms_ref, out_terms), (rows_ref, out_rows), (loss_ref, out_loss))
    copies = [pltpu.make_async_copy(a, b, sems.at[i]) for i, (a, b) in enumerate(pairs)]
    for copy in copies:
        copy.start()
    for copy in copies:
        copy.wait()


def on_device(n, n_group, features, weight, owner, slots, queries, ways):
    rows = features.shape[0]
    chips = n // 2
    lines = D * D // LANES
    vmem = pl.BlockSpec(memory_space=pltpu.VMEM)
    dma = pltpu.SemaphoreType.DMA
    side = math.isqrt(chips)
    part = (2, side, lines // (2 * side), LANES)
    hbm = pl.BlockSpec(memory_space=pl.ANY)
    own_rows, terms, losses = pl.pallas_call(
        functools.partial(kernel, n, n_group),
        out_shape=(
            pltpu.VMEM((rows, D), BF16),
            pltpu.VMEM((D, D), F32),
            pltpu.VMEM((1, 1), F32),
        ),
        in_specs=[hbm] * 6,
        out_specs=(vmem, vmem, vmem),
        scratch_shapes=[
            pltpu.VMEM((1, rows), I32),
            pltpu.VMEM((1, rows), I32),
            pltpu.VMEM((1, rows), I32),
            pltpu.VMEM((1, 1), I32),
            pltpu.VMEM((rows, D), BF16),
            pltpu.VMEM((D, D), BF16),
            pltpu.VMEM((1, n), F32),
            pltpu.VMEM((2 * side, 1, n), F32),
            pltpu.VMEM((side, 2 * side, 1, n), F32),
            pltpu.VMEM((2 * side, side, CAP, D // 2), BF16),
            pltpu.VMEM((side, 2 * side, CAP, D // 2), BF16),
            pltpu.VMEM((side, 2 * side, CAP, D // 2), BF16),
            pltpu.VMEM((side, 2 * side, CAP, D // 2), BF16),
            pltpu.VMEM((2 * side, side, CAP, D // 2), BF16),
            pltpu.VMEM((side, 2 * side, CAP, D // 2), BF16),
            pltpu.VMEM((n, CAP, D), BF16),
            pltpu.VMEM((n, CAP, D), BF16),
            pltpu.VMEM((2, n * CAP, D // 2), BF16),
            pltpu.VMEM((2, lines // 2, LANES), BF16),
            pltpu.VMEM((2, lines // 2, LANES), BF16),
            pltpu.VMEM(part, BF16),
            pltpu.VMEM(part, BF16),
            pltpu.VMEM((2, *part[2:]), BF16),
            pltpu.VMEM(part, BF16),
            pltpu.VMEM((2, *part[2:]), BF16),
            pltpu.VMEM((2, n_group, *part[2:]), BF16),
            pltpu.VMEM(part, BF16),
            pltpu.SemaphoreType.DMA((6,)),
        ]
        + [pltpu.SemaphoreType.DMA((2,))] * 6
        + [dma] * 2
        + [pltpu.SemaphoreType.DMA((2,))] * 12
        + [pltpu.SemaphoreType.REGULAR],
        compiler_params=pltpu.CompilerParams(collective_id=0, has_side_effects=True),
        name="episodes",
    )(
        owner.reshape(1, rows),
        slots.reshape(1, rows),
        queries.reshape(1, rows),
        ways.reshape(1, 1),
        features,
        weight,
    )
    own_rows, terms, losses = pl.pallas_call(
        put_out,
        out_shape=(
            jax.ShapeDtypeStruct((rows, D), BF16),
            jax.ShapeDtypeStruct((D, D), F32),
            jax.ShapeDtypeStruct((1, 1), F32),
        ),
        in_specs=[vmem] * 3,
        out_specs=(hbm, hbm, hbm),
        scratch_shapes=[pltpu.SemaphoreType.DMA((3,))],
        name="results",
    )(*(pltpu.with_memory_space_constraint(x, pltpu.VMEM) for x in (own_rows, terms, losses)))
    return own_rows, terms, losses.reshape(1)


def solution(mesh):
    both = P(("dp", "group"))
    lines = P(("dp", "group"), None)
    return jax.shard_map(
        functools.partial(on_device, mesh.shape["dp"], mesh.shape["group"]),
        mesh=mesh,
        in_specs=(lines, P(), lines, both, both, both),
        out_specs=(lines, P(), both),
        check_vma=False,
    )
```

```python
import functools
import math

import jax
import jax.numpy as jnp
from jax import lax
from jax.experimental import pallas as pl
from jax.experimental.pallas import tpu as pltpu
from jax.sharding import PartitionSpec as P

D = 512
WAYS_MAX = 50
CLASSES = 64
CAP = 2
LANES = 128
MESH = pl.DeviceIdType.MESH
F32 = jnp.float32
BF16 = jnp.bfloat16
I32 = jnp.int32
BACK = ((0, 0, 64, 127), (0, 127, 127))
WAIT = (0, 2500)


def dot(a, b, ca, cb):
    return lax.dot_general(a, b, (((ca,), (cb,)), ((), ())), preferred_element_type=F32)


def iota(shape, dim):
    return lax.broadcasted_iota(I32, shape, dim)


def three_parts(x):
    hi = x.astype(BF16)
    rest = x - hi.astype(F32)
    mid = rest.astype(BF16)
    low = (rest - mid.astype(F32)).astype(BF16)
    return hi, mid, low


def to_lanes(column):
    n = column.shape[0]
    same = iota((n, n), 0) == iota((n, n), 1)
    return jnp.sum(jnp.where(same, column, 0.0), axis=0, keepdims=True)


def to_sublanes(row):
    n = row.shape[1]
    same = iota((n, n), 0) == iota((n, n), 1)
    return jnp.sum(jnp.where(same, row, 0.0), axis=1, keepdims=True)


def episode(rows, codes, ways, weight):
    count = rows.shape[0]
    embeds = dot(rows, weight, 1, 0).astype(BF16)
    wide = embeds.astype(F32)
    code = codes.astype(I32)
    value = jnp.maximum(code - 1, 0)
    live = code > 0
    odd = lax.rem(value, 2) == 1
    query = (live & odd).astype(F32)
    label = lax.div(value, 2)
    for factor in (8, 4, 2, 1):
        label = jnp.where(label >= factor * ways, label - factor * ways, label)
    classes = iota((CLASSES, count), 0)
    hot = classes == label
    support = jnp.where(hot & live & jnp.logical_not(odd), 1.0, 0.0)
    counts = jnp.maximum(jnp.sum(support, axis=1, keepdims=True), 1.0)
    support = support.astype(BF16)
    protos = dot(support, embeds, 1, 0) / counts
    parts = three_parts(protos)
    crosses = dot(jnp.concatenate(parts, axis=0), embeds, 1, 1)
    cross = crosses[:CLASSES] + crosses[CLASSES : 2 * CLASSES] + crosses[2 * CLASSES :]
    norm_e = to_lanes(jnp.sum(wide * wide, axis=1, keepdims=True))
    norm_p = jnp.sum(protos * protos, axis=1, keepdims=True)
    distance = norm_e - 2.0 * cross + norm_p
    scores = -distance * D ** (-0.5)
    masked = jnp.where(classes < ways, scores, -1e30)
    top = jnp.max(masked, axis=0, keepdims=True)
    powers = jnp.exp(masked - top)
    total = jnp.sum(powers, axis=0, keepdims=True)
    picked = jnp.sum(jnp.where(hot, scores, 0.0), axis=0, keepdims=True)
    per_query = jnp.where(query > 0.0, top + jnp.log(total) - picked, 0.0)
    queries = jnp.maximum(jnp.sum(query, axis=1, keepdims=True), 1.0)
    loss = jnp.sum(per_query, axis=1, keepdims=True) / queries
    share = query / queries
    by_dist = (jnp.where(hot, 1.0, 0.0) - powers / total) * (share * D ** (-0.5))
    by_parts = three_parts(by_dist)
    pulls = dot(jnp.concatenate(by_parts, axis=0), embeds, 1, 0)
    pull = pulls[:CLASSES] + pulls[CLASSES : 2 * CLASSES] + pulls[2 * CLASSES :]
    by_sums = 2.0 * (protos * jnp.sum(by_dist, axis=1, keepdims=True) - pull) / counts
    sum_parts = three_parts(by_sums)
    left = jnp.concatenate([by_parts[0], by_parts[0], by_parts[1], support, support], axis=0)
    right = jnp.concatenate(
        [-2.0 * parts[0], -2.0 * parts[1], -2.0 * parts[0], sum_parts[0], sum_parts[1]], axis=0
    )
    own = to_sublanes(jnp.sum(by_dist, axis=0, keepdims=True))
    grads = dot(left, right, 0, 0) + 2.0 * own * wide
    return grads.astype(BF16), loss


def farthest_first(count):
    return sorted(range(count), key=lambda i: -min(i, count - i))


def one_hot(places, count):
    return jnp.where(iota((count, places.shape[1]), 0) == places, 1.0, 0.0).astype(BF16)


def arrived(block, sem):
    pltpu.make_async_copy(block, block, sem).wait()


def lay_out(blocks, out_ref, which):
    lines = out_ref.shape[0] // 2
    value = blocks[which].reshape(D // LANES, lines, LANES)
    start = which * lines
    for i in range(D // LANES):
        out_ref[start : start + lines, i * LANES : (i + 1) * LANES] = value[i].astype(F32)


def kernel(
    n,
    n_group,
    owner_hbm,
    slot_hbm,
    query_hbm,
    ways_hbm,
    features_hbm,
    weight_hbm,
    out_rows_ref,
    out_weight_ref,
    out_loss_ref,
    owner_ref,
    slot_ref,
    query_ref,
    ways_ref,
    features_ref,
    weight_ref,
    code_send,
    code_mid,
    code_recv,
    left_send,
    left_mid,
    left_recv,
    right_send,
    right_mid,
    right_recv,
    back_send,
    back_recv,
    halves,
    fold_send,
    fold_recv,
    part_send,
    part_recv,
    line_send,
    line_recv,
    cross_send,
    cross_recv,
    whole,
    load_sem,
    code_ss,
    code_rs,
    left_ss,
    left_rs,
    right_ss,
    right_rs,
    back_ss,
    back_rs,
    pair_ss,
    pair_rs,
    part_ss,
    part_rs,
    line_ss,
    line_rs,
    cross_ss,
    cross_rs,
    whole_ss,
    whole_rs,
    tick,
):
    me = lax.axis_index("dp")
    group = lax.axis_index("group")
    chips = n // 2
    side = math.isqrt(chips)
    core = lax.rem(me, 2)
    chip = lax.div(me, 2)
    high = lax.div(chip, side)
    low = lax.rem(chip, side)
    twin = me + 1 - 2 * core
    rows = features_ref.shape[0]
    half = D // 2
    offsets = farthest_first(side)
    highs = [lax.rem(high + i, side) * (2 * side) for i in range(side)]
    lows = [lax.rem(low + i, side) * 2 for i in range(side)]
    wide = 2 * side
    mine = 2 * low + core
    row_line = [(2 * lax.rem(low + i, side) + c, highs[0] + lows[i] + c) for i in offsets if i for c in range(2)]
    row_line.append((mine + 1 - 2 * core, twin))
    groups = [lax.rem(group + i, n_group) for i in range(1, n_group)]
    plane = [(h, w) for h in offsets for w in offsets if h or w]
    row_peers = [highs[h] + lows[w] + c for h, w in plane for c in range(2)] + [twin]
    lines = [
        (low, [(lax.rem(low + i, side), highs[0] + lows[i] + core) for i in offsets if i]),
        (high, [(lax.rem(high + i, side), highs[i] + lows[0] + core) for i in offsets if i]),
    ]

    barrier = pltpu.get_barrier_semaphore()
    with jax.named_scope("greet"):
        for _, peer in row_line + lines[1][1]:
            pl.semaphore_signal(barrier, inc=1, device_id=(peer, group), device_id_type=MESH)
        for peer in groups:
            pl.semaphore_signal(barrier, inc=1, device_id=(me, peer), device_id_type=MESH)
    pairs = (
        (owner_hbm, owner_ref, 0),
        (slot_hbm, slot_ref, 0),
        (query_hbm, query_ref, 0),
        (features_hbm, features_ref, 1),
        (ways_hbm, ways_ref, 2),
        (weight_hbm, weight_ref, 3),
    )
    loads = [pltpu.make_async_copy(source, target, load_sem.at[i]) for source, target, i in pairs]
    for load in loads:
        load.start()
    arrived(code_mid.at[pl.ds(0, 3)], load_sem.at[0])
    for load in loads[3:]:
        load.wait()

    owner_lane = owner_ref[...].astype(F32)
    owner = to_sublanes(owner_lane)
    earlier = (owner == owner_lane) & (iota((rows, rows), 0) < iota((rows, rows), 1))
    place = jnp.sum(jnp.where(earlier, 1.0, 0.0), axis=0, keepdims=True)
    codes = (slot_ref[...] * 2 + query_ref[...] + 1).astype(F32)
    weighed = to_sublanes(codes * jnp.where(place > 0.0, 1.0 * LANES, 1.0))
    code_send[...] = jnp.sum(
        jnp.where(owner == iota((rows, n), 1).astype(F32), weighed, 0.0), axis=0, keepdims=True
    )
    code_mid[mine] = code_send[...]
    target = owner_lane.astype(I32)
    place = place.astype(I32)
    hot = one_hot(target * CAP + place, n * CAP)
    turned = (lax.rem(target, wide) * side + lax.div(target, wide)) * CAP + place
    left = dot(one_hot(turned, n * CAP), features_ref[:, :half], 1, 0).astype(BF16)
    left_send[...] = left.reshape(left_send.shape)
    right = dot(hot, features_ref[:, half:], 1, 0).astype(BF16)
    right_send[...] = right.reshape(right_send.shape)
    left_mid[:, mine] = left_send[mine]
    right_mid[:, high] = right_send[high]

    with jax.named_scope("barrier_wait"):
        pl.semaphore_wait(barrier, wide + side + n_group - 3)

    def push(source, target, send_sem, recv_sem, peer):
        pltpu.make_async_remote_copy(
            src_ref=source,
            dst_ref=target,
            send_sem=send_sem,
            recv_sem=recv_sem,
            device_id=(peer, group),
            device_id_type=MESH,
        ).start()

    with jax.named_scope("send_rows"):
        for place, peer in row_line:
            push(code_send, code_mid.at[mine], code_ss, code_rs.at[0], peer)
        for place, peer in row_line:
            push(left_send.at[place], left_mid.at[:, mine], left_ss, left_rs.at[0], peer)
        for place, peer in lines[1][1]:
            push(right_send.at[place], right_mid.at[:, high], right_ss, right_rs.at[0], peer)
    with jax.named_scope("code_wait0"):
        arrived(code_mid.at[pl.ds(0, wide - 1)], code_rs.at[0])
    for place, peer in lines[1][1]:
        push(code_mid, code_recv.at[pl.ds(high * wide, wide)], code_ss, code_rs.at[1], peer)
    code_recv[pl.ds(high * wide, wide)] = code_mid[...]
    with jax.named_scope("left_wait0"):
        arrived(left_mid.at[:, pl.ds(0, wide - 1)], left_rs.at[0])
    for place, peer in lines[1][1]:
        push(left_mid.at[place], left_recv.at[high], left_ss, left_rs.at[1], peer)
    left_recv[high] = left_mid[high]
    with jax.named_scope("right_wait0"):
        arrived(right_mid.at[:, pl.ds(0, side - 1)], right_rs.at[0])
    for place, peer in row_line:
        push(right_mid.at[place], right_recv.at[:, mine], right_ss, right_rs.at[1], peer)
    right_recv[:, mine] = right_mid[mine]
    with jax.named_scope("code_wait1"):
        arrived(code_recv.at[pl.ds(0, n - wide)], code_rs.at[1])
    table = code_recv[...].reshape(n, n)
    both = jnp.sum(jnp.where(iota((n, n), 1) == me, table, 0.0), axis=1, keepdims=True).astype(I32)
    spot = iota((n, n * CAP), 1)
    chosen = jnp.where(lax.rem(spot, CAP) == 0, lax.rem(both, LANES), lax.div(both, LANES))
    chosen = jnp.where(lax.div(spot, CAP) == iota((n, n * CAP), 0), chosen, 0)
    got_codes = jnp.sum(chosen.astype(F32), axis=0, keepdims=True)
    with jax.named_scope("left_wait1"):
        arrived(left_recv.at[pl.ds(0, side - 1)], left_rs.at[1])
    halves[0] = left_recv[...].reshape(n * CAP, half)
    with jax.named_scope("right_wait1"):
        arrived(right_recv.at[:, pl.ds(0, wide - 1)], right_rs.at[1])
    halves[1] = right_recv[...].reshape(n * CAP, half)
    got_rows = jnp.concatenate([halves[0], halves[1]], axis=1)
    with jax.named_scope("episode"):
        grads, loss = episode(got_rows, got_codes, ways_ref[...], weight_ref[...])
        out_loss_ref[...] = loss

    def term(which):
        value = dot(halves[which], grads, 0, 0)
        return jnp.concatenate(
            [value[:, i * LANES : (i + 1) * LANES] for i in range(D // LANES)], axis=0
        )

    def fold(which):
        return pltpu.make_async_remote_copy(
            src_ref=fold_send.at[which],
            dst_ref=fold_recv.at[which],
            send_sem=pair_ss,
            recv_sem=pair_rs.at[which],
            device_id=(twin, group),
            device_id_type=MESH,
        )

    def last(which):
        return pltpu.make_async_remote_copy(
            src_ref=whole.at[which],
            dst_ref=whole.at[which],
            send_sem=pair_ss,
            recv_sem=pair_rs.at[which],
            device_id=(twin, group),
            device_id_type=MESH,
        )

    def prepare_back():
        outgoing = dot(grads, weight_ref[...], 1, 1).astype(BF16)
        back_send[...] = outgoing.reshape(back_send.shape)
        back_recv[me] = back_send[me]

    def send_back(which, piece):
        with jax.named_scope(f"send_back{piece}"):
            for peer in row_peers[BACK[which][piece] : BACK[which][piece + 1]]:
                push(back_send.at[peer], back_recv.at[me], back_ss, back_rs, peer)

    def take_back():
        with jax.named_scope("back_wait"):
            arrived(back_recv.at[pl.ds(0, n - 1)], back_rs)
        returned = back_recv[...].reshape(n * CAP, D)
        out_rows_ref[...] = dot(hot, returned, 0, 0).astype(BF16)

    def spread(axis, source, target, send_sem, recv_sem):
        for place, peer in lines[axis][1]:
            push(source(place), target, send_sem, recv_sem, peer)

    def tell():
        pl.semaphore_signal(tick, inc=1, device_id=(twin, group), device_id_type=MESH)

    @pl.when(core == 1)
    def _():
        own = [term(0), term(1)]
        prepare_back()
        for i in range(2):
            with jax.named_scope(f"fold_wait{i}"):
                fold(i).wait_recv()
            total = own[i] + fold_recv[i].astype(F32)
            part_send[i] = total.astype(BF16).reshape(part_send.shape[1:])
            here = lines[i][0]
            spread(i, lambda p: part_send.at[i, p], part_recv.at[i, here], part_ss, part_rs.at[i])
            part_recv[i, here] = part_send[i, here]
        for i in range(2):
            with jax.named_scope(f"part_wait{i}"):
                arrived(part_recv.at[i, pl.ds(0, side - 1)], part_rs.at[i])
            line_send[i] = jnp.sum(part_recv[i].astype(F32), axis=0).astype(BF16)
            here = lines[1 - i][0]
            spread(1 - i, lambda p: line_send.at[i], line_recv.at[i, here], line_ss, line_rs.at[i])
            line_recv[i, here] = line_send[i]
        tell()
        send_back(1, 0)
        for i in range(2):
            with jax.named_scope(f"line_wait{i}"):
                arrived(line_recv.at[i, pl.ds(0, side - 1)], line_rs.at[i])
            cross_send[i] = jnp.sum(line_recv[i].astype(F32), axis=0).astype(BF16)
            for peer in groups:
                pltpu.make_async_remote_copy(
                    src_ref=cross_send.at[i],
                    dst_ref=cross_recv.at[i, group],
                    send_sem=cross_ss,
                    recv_sem=cross_rs.at[i],
                    device_id=(me, peer),
                    device_id_type=MESH,
                ).start()
            cross_recv[i, group] = cross_send[i]
        tell()
        send_back(1, 1)
        for i in range(2):
            with jax.named_scope(f"cross_wait{i}"):
                arrived(cross_recv.at[i, pl.ds(0, n_group - 1)], cross_rs.at[i])
            here = lines[i][0]
            whole[i, here] = jnp.sum(cross_recv[i].astype(F32), axis=0).astype(BF16)
            final = whole.at[i, here]
            spread(i, lambda p: final, final, whole_ss, whole_rs.at[i])
        for i in range(2):
            with jax.named_scope(f"whole_wait{i}"):
                arrived(whole.at[i, pl.ds(0, side - 1)], whole_rs.at[i])
            last(i).start()
        for i in range(2):
            lay_out(whole, out_weight_ref, i)
        take_back()
        arrived(part_recv.at[:, pl.ds(0, side - 1)], part_ss)
        arrived(line_recv.at[:, pl.ds(0, side - 1)], line_ss)
        arrived(cross_recv.at[:, pl.ds(0, n_group - 1)], cross_ss)
        arrived(whole.at[:, pl.ds(0, side - 1)], whole_ss)
        arrived(whole, pair_ss)

    @pl.when(core == 0)
    def _():
        for i in range(2):
            fold_send[i] = term(i).astype(BF16)
            fold(i).start()
        prepare_back()
        if WAIT[0]:
            pl.delay(WAIT[0])
        send_back(0, 0)
        with jax.named_scope("tick_wait0"):
            pl.semaphore_wait(tick, 1)
        if WAIT[1]:
            pl.delay(WAIT[1])
        send_back(0, 1)
        with jax.named_scope("tick_wait1"):
            pl.semaphore_wait(tick, 1)
        send_back(0, 2)
        take_back()
        for i in range(2):
            with jax.named_scope(f"last_wait{i}"):
                last(i).wait_recv()
            lay_out(whole, out_weight_ref, i)
        arrived(fold_send, pair_ss)

    arrived(code_recv.at[pl.ds(0, n - 1)], code_ss)
    sent = ((wide - 1) * side + (side - 1) * wide) // 2
    arrived(back_send.at[pl.ds(0, sent)], left_ss)
    arrived(back_send.at[pl.ds(0, sent)], right_ss)
    arrived(back_send.at[pl.ds(0, n - 1)], back_ss)


def put_out(rows_ref, terms_ref, loss_ref, out_rows, out_terms, out_loss, sems):
    pieces = 8
    lines = terms_ref.shape[0] // pieces
    for i in range(pieces):
        block = pl.ds(i * lines, lines)
        pltpu.make_async_copy(terms_ref.at[block], out_terms.at[block], sems.at[0]).start()
    others = [
        pltpu.make_async_copy(rows_ref, out_rows, sems.at[1]),
        pltpu.make_async_copy(loss_ref, out_loss, sems.at[2]),
    ]
    for copy in others:
        copy.start()
    arrived(terms_ref, sems.at[0])
    for copy in others:
        copy.wait()


def on_device(n, n_group, features, weight, owner, slots, queries, ways):
    rows = features.shape[0]
    chips = n // 2
    lines = D * D // LANES
    vmem = pl.BlockSpec(memory_space=pltpu.VMEM)
    dma = pltpu.SemaphoreType.DMA
    two = pltpu.SemaphoreType.DMA((2,))
    side = math.isqrt(chips)
    part = (2, side, lines // (2 * side), LANES)
    hbm = pl.BlockSpec(memory_space=pl.ANY)
    own_rows, terms, losses = pl.pallas_call(
        functools.partial(kernel, n, n_group),
        out_shape=(
            pltpu.VMEM((rows, D), BF16),
            pltpu.VMEM((D, D), F32),
            pltpu.VMEM((1, 1), F32),
        ),
        in_specs=[hbm] * 6,
        out_specs=(vmem, vmem, vmem),
        scratch_shapes=[
            pltpu.VMEM((1, rows), I32),
            pltpu.VMEM((1, rows), I32),
            pltpu.VMEM((1, rows), I32),
            pltpu.VMEM((1, 1), I32),
            pltpu.VMEM((rows, D), BF16),
            pltpu.VMEM((D, D), BF16),
            pltpu.VMEM((1, n), F32),
            pltpu.VMEM((2 * side, 1, n), F32),
            pltpu.VMEM((n, 1, n), F32),
            pltpu.VMEM((2 * side, side, CAP, D // 2), BF16),
            pltpu.VMEM((side, 2 * side, CAP, D // 2), BF16),
            pltpu.VMEM((side, 2 * side, CAP, D // 2), BF16),
            pltpu.VMEM((side, 2 * side, CAP, D // 2), BF16),
            pltpu.VMEM((2 * side, side, CAP, D // 2), BF16),
            pltpu.VMEM((side, 2 * side, CAP, D // 2), BF16),
            pltpu.VMEM((n, CAP, D), BF16),
            pltpu.VMEM((n, CAP, D), BF16),
            pltpu.VMEM((2, n * CAP, D // 2), BF16),
            pltpu.VMEM((2, lines // 2, LANES), BF16),
            pltpu.VMEM((2, lines // 2, LANES), BF16),
            pltpu.VMEM(part, BF16),
            pltpu.VMEM(part, BF16),
            pltpu.VMEM((2, *part[2:]), BF16),
            pltpu.VMEM(part, BF16),
            pltpu.VMEM((2, *part[2:]), BF16),
            pltpu.VMEM((2, n_group, *part[2:]), BF16),
            pltpu.VMEM(part, BF16),
            pltpu.SemaphoreType.DMA((4,)),
        ]
        + [dma, two] * 3
        + [dma, dma]
        + [dma, two] * 5
        + [pltpu.SemaphoreType.REGULAR],
        compiler_params=pltpu.CompilerParams(collective_id=0, has_side_effects=True),
        name="episodes",
    )(
        owner.reshape(1, rows),
        slots.reshape(1, rows),
        queries.reshape(1, rows),
        ways.reshape(1, 1),
        features,
        weight,
    )
    own_rows, terms, losses = pl.pallas_call(
        put_out,
        out_shape=(
            jax.ShapeDtypeStruct((rows, D), BF16),
            jax.ShapeDtypeStruct((D, D), F32),
            jax.ShapeDtypeStruct((1, 1), F32),
        ),
        in_specs=[vmem] * 3,
        out_specs=(hbm, hbm, hbm),
        scratch_shapes=[pltpu.SemaphoreType.DMA((3,))],
        name="results",
    )(*(pltpu.with_memory_space_constraint(x, pltpu.VMEM) for x in (own_rows, terms, losses)))
    return own_rows, terms, losses.reshape(1)


def solution(mesh):
    both = P(("dp", "group"))
    lines = P(("dp", "group"), None)
    return jax.shard_map(
        functools.partial(on_device, mesh.shape["dp"], mesh.shape["group"]),
        mesh=mesh,
        in_specs=(lines, P(), lines, both, both, both),
        out_specs=(lines, P(), both),
        check_vma=False,
    )
```

```python
import functools
import math

import jax
import jax.numpy as jnp
from jax import lax
from jax.experimental import pallas as pl
from jax.experimental.pallas import tpu as pltpu
from jax.sharding import PartitionSpec as P

D = 512
WAYS_MAX = 50
CLASSES = 64
CAP = 2
LANES = 128
MESH = pl.DeviceIdType.MESH
F32 = jnp.float32
BF16 = jnp.bfloat16
I32 = jnp.int32
BACK = ((0, 127, 127), (0, 127))
WAIT = (4000, 0)


def dot(a, b, ca, cb):
    return lax.dot_general(a, b, (((ca,), (cb,)), ((), ())), preferred_element_type=F32)


def iota(shape, dim):
    return lax.broadcasted_iota(I32, shape, dim)


def three_parts(x):
    hi = x.astype(BF16)
    rest = x - hi.astype(F32)
    mid = rest.astype(BF16)
    low = (rest - mid.astype(F32)).astype(BF16)
    return hi, mid, low


def to_lanes(column):
    n = column.shape[0]
    same = iota((n, n), 0) == iota((n, n), 1)
    return jnp.sum(jnp.where(same, column, 0.0), axis=0, keepdims=True)


def to_sublanes(row):
    n = row.shape[1]
    same = iota((n, n), 0) == iota((n, n), 1)
    return jnp.sum(jnp.where(same, row, 0.0), axis=1, keepdims=True)


def episode(rows, codes, ways, weight):
    count = rows.shape[0]
    embeds = dot(rows, weight, 1, 0).astype(BF16)
    wide = embeds.astype(F32)
    code = codes.astype(I32)
    value = jnp.maximum(code - 1, 0)
    live = code > 0
    odd = lax.rem(value, 2) == 1
    query = (live & odd).astype(F32)
    label = lax.div(value, 2)
    for factor in (8, 4, 2, 1):
        label = jnp.where(label >= factor * ways, label - factor * ways, label)
    classes = iota((CLASSES, count), 0)
    hot = classes == label
    support = jnp.where(hot & live & jnp.logical_not(odd), 1.0, 0.0)
    counts = jnp.maximum(jnp.sum(support, axis=1, keepdims=True), 1.0)
    support = support.astype(BF16)
    protos = dot(support, embeds, 1, 0) / counts
    parts = three_parts(protos)
    crosses = dot(jnp.concatenate(parts, axis=0), embeds, 1, 1)
    cross = crosses[:CLASSES] + crosses[CLASSES : 2 * CLASSES] + crosses[2 * CLASSES :]
    norm_e = to_lanes(jnp.sum(wide * wide, axis=1, keepdims=True))
    norm_p = jnp.sum(protos * protos, axis=1, keepdims=True)
    distance = norm_e - 2.0 * cross + norm_p
    scores = -distance * D ** (-0.5)
    masked = jnp.where(classes < ways, scores, -1e30)
    top = jnp.max(masked, axis=0, keepdims=True)
    powers = jnp.exp(masked - top)
    total = jnp.sum(powers, axis=0, keepdims=True)
    picked = jnp.sum(jnp.where(hot, scores, 0.0), axis=0, keepdims=True)
    per_query = jnp.where(query > 0.0, top + jnp.log(total) - picked, 0.0)
    queries = jnp.maximum(jnp.sum(query, axis=1, keepdims=True), 1.0)
    loss = jnp.sum(per_query, axis=1, keepdims=True) / queries
    share = query / queries
    by_dist = (jnp.where(hot, 1.0, 0.0) - powers / total) * (share * D ** (-0.5))
    by_parts = three_parts(by_dist)
    pulls = dot(jnp.concatenate(by_parts, axis=0), embeds, 1, 0)
    pull = pulls[:CLASSES] + pulls[CLASSES : 2 * CLASSES] + pulls[2 * CLASSES :]
    by_sums = 2.0 * (protos * jnp.sum(by_dist, axis=1, keepdims=True) - pull) / counts
    sum_parts = three_parts(by_sums)
    left = jnp.concatenate([by_parts[0], by_parts[0], by_parts[1], support, support], axis=0)
    right = jnp.concatenate(
        [-2.0 * parts[0], -2.0 * parts[1], -2.0 * parts[0], sum_parts[0], sum_parts[1]], axis=0
    )
    own = to_sublanes(jnp.sum(by_dist, axis=0, keepdims=True))
    grads = dot(left, right, 0, 0) + 2.0 * own * wide
    return grads.astype(BF16), loss


def farthest_first(count):
    return sorted(range(count), key=lambda i: -min(i, count - i))


def one_hot(places, count):
    return jnp.where(iota((count, places.shape[1]), 0) == places, 1.0, 0.0).astype(BF16)


def arrived(block, sem):
    pltpu.make_async_copy(block, block, sem).wait()


def lay_out(blocks, out_ref, which):
    lines = out_ref.shape[0] // 2
    value = blocks[which].reshape(D // LANES, lines, LANES)
    start = which * lines
    for i in range(D // LANES):
        out_ref[start : start + lines, i * LANES : (i + 1) * LANES] = value[i].astype(F32)


def kernel(
    n,
    n_group,
    owner_hbm,
    slot_hbm,
    query_hbm,
    ways_hbm,
    features_hbm,
    weight_hbm,
    out_rows_ref,
    out_weight_ref,
    out_loss_ref,
    owner_ref,
    slot_ref,
    query_ref,
    ways_ref,
    features_ref,
    weight_ref,
    code_send,
    code_mid,
    code_recv,
    left_send,
    left_mid,
    left_recv,
    right_send,
    right_mid,
    right_recv,
    back_send,
    back_recv,
    halves,
    fold_send,
    fold_recv,
    part_send,
    part_recv,
    line_send,
    line_recv,
    whole,
    load_sem,
    code_ss,
    code_rs,
    left_ss,
    left_rs,
    right_ss,
    right_rs,
    back_ss,
    back_rs,
    pair_ss,
    pair_rs,
    part_ss,
    part_rs,
    line_ss,
    line_rs,
    whole_ss,
    whole_rs,
    tick,
):
    me = lax.axis_index("dp")
    group = lax.axis_index("group")
    chips = n // 2
    side = math.isqrt(chips)
    spots = side * n_group
    core = lax.rem(me, 2)
    chip = lax.div(me, 2)
    high = lax.div(chip, side)
    low = lax.rem(chip, side)
    twin = me + 1 - 2 * core
    rows = features_ref.shape[0]
    half = D // 2
    offsets = farthest_first(side)
    highs = [lax.rem(high + i, side) * (2 * side) for i in range(side)]
    lows = [lax.rem(low + i, side) * 2 for i in range(side)]
    wide = 2 * side
    mine = 2 * low + core
    row_line = [(2 * lax.rem(low + i, side) + c, highs[0] + lows[i] + c) for i in offsets if i for c in range(2)]
    row_line.append((mine + 1 - 2 * core, twin))
    groups = [lax.rem(group + i, n_group) for i in range(1, n_group)]
    plane = [(h, w) for h in offsets for w in offsets if h or w]
    row_peers = [highs[h] + lows[w] + c for h, w in plane for c in range(2)] + [twin]
    lines = [
        (low, [(lax.rem(low + i, side), highs[0] + lows[i] + core) for i in offsets if i]),
        (high, [(lax.rem(high + i, side), highs[i] + lows[0] + core) for i in offsets if i]),
    ]

    barrier = pltpu.get_barrier_semaphore()
    with jax.named_scope("greet"):
        for _, peer in row_line + lines[1][1]:
            pl.semaphore_signal(barrier, inc=1, device_id=(peer, group), device_id_type=MESH)
        for peer in groups:
            pl.semaphore_signal(barrier, inc=1, device_id=(me, peer), device_id_type=MESH)
    pairs = (
        (owner_hbm, owner_ref, 0),
        (slot_hbm, slot_ref, 0),
        (query_hbm, query_ref, 0),
        (features_hbm, features_ref, 1),
        (ways_hbm, ways_ref, 2),
        (weight_hbm, weight_ref, 3),
    )
    loads = [pltpu.make_async_copy(source, target, load_sem.at[i]) for source, target, i in pairs]
    for load in loads:
        load.start()
    arrived(code_mid.at[pl.ds(0, 3)], load_sem.at[0])
    for load in loads[3:]:
        load.wait()

    owner_lane = owner_ref[...].astype(F32)
    owner = to_sublanes(owner_lane)
    earlier = (owner == owner_lane) & (iota((rows, rows), 0) < iota((rows, rows), 1))
    place = jnp.sum(jnp.where(earlier, 1.0, 0.0), axis=0, keepdims=True)
    codes = (slot_ref[...] * 2 + query_ref[...] + 1).astype(F32)
    weighed = to_sublanes(codes * jnp.where(place > 0.0, 1.0 * LANES, 1.0))
    code_send[...] = jnp.sum(
        jnp.where(owner == iota((rows, n), 1).astype(F32), weighed, 0.0), axis=0, keepdims=True
    )
    code_mid[mine] = code_send[...]
    target = owner_lane.astype(I32)
    place = place.astype(I32)
    hot = one_hot(target * CAP + place, n * CAP)
    turned = (lax.rem(target, wide) * side + lax.div(target, wide)) * CAP + place
    left = dot(one_hot(turned, n * CAP), features_ref[:, :half], 1, 0).astype(BF16)
    left_send[...] = left.reshape(left_send.shape)
    right = dot(hot, features_ref[:, half:], 1, 0).astype(BF16)
    right_send[...] = right.reshape(right_send.shape)
    left_mid[:, mine] = left_send[mine]
    right_mid[:, high] = right_send[high]

    with jax.named_scope("barrier_wait"):
        pl.semaphore_wait(barrier, wide + side + n_group - 3)

    def push(source, target, send_sem, recv_sem, peer):
        pltpu.make_async_remote_copy(
            src_ref=source,
            dst_ref=target,
            send_sem=send_sem,
            recv_sem=recv_sem,
            device_id=(peer, group),
            device_id_type=MESH,
        ).start()

    with jax.named_scope("send_rows"):
        for place, peer in row_line:
            push(code_send, code_mid.at[mine], code_ss, code_rs.at[0], peer)
        for place, peer in row_line:
            push(left_send.at[place], left_mid.at[:, mine], left_ss, left_rs.at[0], peer)
        for place, peer in lines[1][1]:
            push(right_send.at[place], right_mid.at[:, high], right_ss, right_rs.at[0], peer)
    with jax.named_scope("code_wait0"):
        arrived(code_mid.at[pl.ds(0, wide - 1)], code_rs.at[0])
    for place, peer in lines[1][1]:
        push(code_mid, code_recv.at[pl.ds(high * wide, wide)], code_ss, code_rs.at[1], peer)
    code_recv[pl.ds(high * wide, wide)] = code_mid[...]
    with jax.named_scope("left_wait0"):
        arrived(left_mid.at[:, pl.ds(0, wide - 1)], left_rs.at[0])
    for place, peer in lines[1][1]:
        push(left_mid.at[place], left_recv.at[high], left_ss, left_rs.at[1], peer)
    left_recv[high] = left_mid[high]
    with jax.named_scope("right_wait0"):
        arrived(right_mid.at[:, pl.ds(0, side - 1)], right_rs.at[0])
    for place, peer in row_line:
        push(right_mid.at[place], right_recv.at[:, mine], right_ss, right_rs.at[1], peer)
    right_recv[:, mine] = right_mid[mine]
    with jax.named_scope("code_wait1"):
        arrived(code_recv.at[pl.ds(0, n - wide)], code_rs.at[1])
    table = code_recv[...].reshape(n, n)
    both = jnp.sum(jnp.where(iota((n, n), 1) == me, table, 0.0), axis=1, keepdims=True).astype(I32)
    spot = iota((n, n * CAP), 1)
    chosen = jnp.where(lax.rem(spot, CAP) == 0, lax.rem(both, LANES), lax.div(both, LANES))
    chosen = jnp.where(lax.div(spot, CAP) == iota((n, n * CAP), 0), chosen, 0)
    got_codes = jnp.sum(chosen.astype(F32), axis=0, keepdims=True)
    with jax.named_scope("left_wait1"):
        arrived(left_recv.at[pl.ds(0, side - 1)], left_rs.at[1])
    halves[0] = left_recv[...].reshape(n * CAP, half)
    with jax.named_scope("right_wait1"):
        arrived(right_recv.at[:, pl.ds(0, wide - 1)], right_rs.at[1])
    halves[1] = right_recv[...].reshape(n * CAP, half)
    got_rows = jnp.concatenate([halves[0], halves[1]], axis=1)
    with jax.named_scope("episode"):
        grads, loss = episode(got_rows, got_codes, ways_ref[...], weight_ref[...])
        out_loss_ref[...] = loss

    def term(which):
        value = dot(halves[which], grads, 0, 0)
        return jnp.concatenate(
            [value[:, i * LANES : (i + 1) * LANES] for i in range(D // LANES)], axis=0
        )

    def fold(which):
        return pltpu.make_async_remote_copy(
            src_ref=fold_send.at[which],
            dst_ref=fold_recv.at[which],
            send_sem=pair_ss,
            recv_sem=pair_rs.at[which],
            device_id=(twin, group),
            device_id_type=MESH,
        )

    def last(which):
        return pltpu.make_async_remote_copy(
            src_ref=whole.at[which],
            dst_ref=whole.at[which],
            send_sem=pair_ss,
            recv_sem=pair_rs.at[which],
            device_id=(twin, group),
            device_id_type=MESH,
        )

    def prepare_back():
        outgoing = dot(grads, weight_ref[...], 1, 1).astype(BF16)
        back_send[...] = outgoing.reshape(back_send.shape)
        back_recv[me] = back_send[me]

    def send_back(which, piece):
        with jax.named_scope(f"send_back{piece}"):
            for peer in row_peers[BACK[which][piece] : BACK[which][piece + 1]]:
                push(back_send.at[peer], back_recv.at[me], back_ss, back_rs, peer)

    def take_back():
        with jax.named_scope("back_wait"):
            arrived(back_recv.at[pl.ds(0, n - 1)], back_rs)
        returned = back_recv[...].reshape(n * CAP, D)
        out_rows_ref[...] = dot(hot, returned, 0, 0).astype(BF16)

    def spread(axis, source, target, send_sem, recv_sem):
        for place, peer in lines[axis][1] + [(lines[axis][0], me)]:
            for other in groups + [group] * (peer is not me):
                pltpu.make_async_remote_copy(
                    src_ref=source(place, other),
                    dst_ref=target,
                    send_sem=send_sem,
                    recv_sem=recv_sem,
                    device_id=(peer, other),
                    device_id_type=MESH,
                ).start()

    def tell():
        pl.semaphore_signal(tick, inc=1, device_id=(twin, group), device_id_type=MESH)

    @pl.when(core == 1)
    def _():
        own = [term(0), term(1)]
        prepare_back()
        for i in range(2):
            with jax.named_scope(f"fold_wait{i}"):
                fold(i).wait_recv()
            total = own[i] + fold_recv[i].astype(F32)
            part_send[i] = total.astype(BF16).reshape(part_send.shape[1:])
            here = lines[i][0] * n_group + group
            spread(i, lambda p, g: part_send.at[i, p * n_group + g], part_recv.at[i, here], part_ss, part_rs.at[i])
            part_recv[i, here] = part_send[i, here]
        for i in range(2):
            with jax.named_scope(f"part_wait{i}"):
                arrived(part_recv.at[i, pl.ds(0, spots - 1)], part_rs.at[i])
            line_send[i] = jnp.sum(part_recv[i].astype(F32), axis=0).astype(BF16)
            here = lines[1 - i][0]
            for _, peer in lines[1 - i][1]:
                push(line_send.at[i], line_recv.at[i, here], line_ss, line_rs.at[i], peer)
            line_recv[i, here] = line_send[i]
        tell()
        send_back(1, 0)
        for i in range(2):
            with jax.named_scope(f"line_wait{i}"):
                arrived(line_recv.at[i, pl.ds(0, side - 1)], line_rs.at[i])
            here = lines[i][0] * n_group + group
            whole[i, here] = jnp.sum(line_recv[i].astype(F32), axis=0).astype(BF16)
            final = whole.at[i, here]
            spread(i, lambda p, g: final, final, whole_ss, whole_rs.at[i])
        for i in range(2):
            with jax.named_scope(f"whole_wait{i}"):
                arrived(whole.at[i, pl.ds(0, spots - 1)], whole_rs.at[i])
            last(i).start()
        for i in range(2):
            lay_out(whole, out_weight_ref, i)
        take_back()
        arrived(part_recv.at[:, pl.ds(0, spots - 1)], part_ss)
        arrived(line_recv.at[:, pl.ds(0, side - 1)], line_ss)
        arrived(whole.at[:, pl.ds(0, spots - 1)], whole_ss)
        arrived(whole, pair_ss)

    @pl.when(core == 0)
    def _():
        for i in range(2):
            fold_send[i] = term(i).astype(BF16)
            fold(i).start()
        prepare_back()
        if WAIT[0]:
            pl.delay(WAIT[0])
        send_back(0, 0)
        with jax.named_scope("tick_wait"):
            pl.semaphore_wait(tick, 1)
        if WAIT[1]:
            pl.delay(WAIT[1])
        send_back(0, 1)
        take_back()
        for i in range(2):
            with jax.named_scope(f"last_wait{i}"):
                last(i).wait_recv()
            lay_out(whole, out_weight_ref, i)
        arrived(fold_send, pair_ss)

    arrived(code_recv.at[pl.ds(0, n - 1)], code_ss)
    sent = ((wide - 1) * side + (side - 1) * wide) // 2
    arrived(back_send.at[pl.ds(0, sent)], left_ss)
    arrived(back_send.at[pl.ds(0, sent)], right_ss)
    arrived(back_send.at[pl.ds(0, n - 1)], back_ss)


def put_out(rows_ref, terms_ref, loss_ref, out_rows, out_terms, out_loss, sems):
    pieces = 8
    lines = terms_ref.shape[0] // pieces
    for i in range(pieces):
        block = pl.ds(i * lines, lines)
        pltpu.make_async_copy(terms_ref.at[block], out_terms.at[block], sems.at[0]).start()
    others = [
        pltpu.make_async_copy(rows_ref, out_rows, sems.at[1]),
        pltpu.make_async_copy(loss_ref, out_loss, sems.at[2]),
    ]
    for copy in others:
        copy.start()
    arrived(terms_ref, sems.at[0])
    for copy in others:
        copy.wait()


def on_device(n, n_group, features, weight, owner, slots, queries, ways):
    rows = features.shape[0]
    chips = n // 2
    lines = D * D // LANES
    vmem = pl.BlockSpec(memory_space=pltpu.VMEM)
    dma = pltpu.SemaphoreType.DMA
    two = pltpu.SemaphoreType.DMA((2,))
    side = math.isqrt(chips)
    part = (2, side * n_group, lines // (2 * side * n_group), LANES)
    hbm = pl.BlockSpec(memory_space=pl.ANY)
    own_rows, terms, losses = pl.pallas_call(
        functools.partial(kernel, n, n_group),
        out_shape=(
            pltpu.VMEM((rows, D), BF16),
            pltpu.VMEM((D, D), F32),
            pltpu.VMEM((1, 1), F32),
        ),
        in_specs=[hbm] * 6,
        out_specs=(vmem, vmem, vmem),
        scratch_shapes=[
            pltpu.VMEM((1, rows), I32),
            pltpu.VMEM((1, rows), I32),
            pltpu.VMEM((1, rows), I32),
            pltpu.VMEM((1, 1), I32),
            pltpu.VMEM((rows, D), BF16),
            pltpu.VMEM((D, D), BF16),
            pltpu.VMEM((1, n), F32),
            pltpu.VMEM((2 * side, 1, n), F32),
            pltpu.VMEM((n, 1, n), F32),
            pltpu.VMEM((2 * side, side, CAP, D // 2), BF16),
            pltpu.VMEM((side, 2 * side, CAP, D // 2), BF16),
            pltpu.VMEM((side, 2 * side, CAP, D // 2), BF16),
            pltpu.VMEM((side, 2 * side, CAP, D // 2), BF16),
            pltpu.VMEM((2 * side, side, CAP, D // 2), BF16),
            pltpu.VMEM((side, 2 * side, CAP, D // 2), BF16),
            pltpu.VMEM((n, CAP, D), BF16),
            pltpu.VMEM((n, CAP, D), BF16),
            pltpu.VMEM((2, n * CAP, D // 2), BF16),
            pltpu.VMEM((2, lines // 2, LANES), BF16),
            pltpu.VMEM((2, lines // 2, LANES), BF16),
            pltpu.VMEM(part, BF16),
            pltpu.VMEM(part, BF16),
            pltpu.VMEM((2, *part[2:]), BF16),
            pltpu.VMEM((2, side, *part[2:]), BF16),
            pltpu.VMEM(part, BF16),
            pltpu.SemaphoreType.DMA((4,)),
        ]
        + [dma, two] * 3
        + [dma, dma]
        + [dma, two] * 4
        + [pltpu.SemaphoreType.REGULAR],
        compiler_params=pltpu.CompilerParams(collective_id=0, has_side_effects=True),
        name="episodes",
    )(
        owner.reshape(1, rows),
        slots.reshape(1, rows),
        queries.reshape(1, rows),
        ways.reshape(1, 1),
        features,
        weight,
    )
    own_rows, terms, losses = pl.pallas_call(
        put_out,
        out_shape=(
            jax.ShapeDtypeStruct((rows, D), BF16),
            jax.ShapeDtypeStruct((D, D), F32),
            jax.ShapeDtypeStruct((1, 1), F32),
        ),
        in_specs=[vmem] * 3,
        out_specs=(hbm, hbm, hbm),
        scratch_shapes=[pltpu.SemaphoreType.DMA((3,))],
        name="results",
    )(*(pltpu.with_memory_space_constraint(x, pltpu.VMEM) for x in (own_rows, terms, losses)))
    return own_rows, terms, losses.reshape(1)


def solution(mesh):
    both = P(("dp", "group"))
    lines = P(("dp", "group"), None)
    return jax.shard_map(
        functools.partial(on_device, mesh.shape["dp"], mesh.shape["group"]),
        mesh=mesh,
        in_specs=(lines, P(), lines, both, both, both),
        out_specs=(lines, P(), both),
        check_vma=False,
    )
```

```python
import functools
import math

import jax
import jax.numpy as jnp
from jax import lax
from jax.experimental import pallas as pl
from jax.experimental.pallas import tpu as pltpu
from jax.sharding import PartitionSpec as P

D = 512
WAYS_MAX = 50
CLASSES = 64
CAP = 2
LANES = 128
MESH = pl.DeviceIdType.MESH
F32 = jnp.float32
BF16 = jnp.bfloat16
I32 = jnp.int32
BACK = ((0, 127, 127), (0, 127))
WAIT = (4000, 0)


def dot(a, b, ca, cb):
    return lax.dot_general(a, b, (((ca,), (cb,)), ((), ())), preferred_element_type=F32)


def iota(shape, dim):
    return lax.broadcasted_iota(I32, shape, dim)


def three_parts(x):
    hi = x.astype(BF16)
    rest = x - hi.astype(F32)
    mid = rest.astype(BF16)
    low = (rest - mid.astype(F32)).astype(BF16)
    return hi, mid, low


def to_lanes(column):
    n = column.shape[0]
    same = iota((n, n), 0) == iota((n, n), 1)
    return jnp.sum(jnp.where(same, column, 0.0), axis=0, keepdims=True)


def to_sublanes(row):
    n = row.shape[1]
    same = iota((n, n), 0) == iota((n, n), 1)
    return jnp.sum(jnp.where(same, row, 0.0), axis=1, keepdims=True)


def episode(rows, codes, ways, weight):
    count = rows.shape[0]
    embeds = dot(rows, weight, 1, 0).astype(BF16)
    wide = embeds.astype(F32)
    code = codes.astype(I32)
    value = jnp.maximum(code - 1, 0)
    live = code > 0
    odd = lax.rem(value, 2) == 1
    query = (live & odd).astype(F32)
    label = lax.div(value, 2)
    for factor in (8, 4, 2, 1):
        label = jnp.where(label >= factor * ways, label - factor * ways, label)
    classes = iota((CLASSES, count), 0)
    hot = classes == label
    support = jnp.where(hot & live & jnp.logical_not(odd), 1.0, 0.0)
    counts = jnp.maximum(jnp.sum(support, axis=1, keepdims=True), 1.0)
    support = support.astype(BF16)
    protos = dot(support, embeds, 1, 0) / counts
    parts = three_parts(protos)
    crosses = dot(jnp.concatenate(parts, axis=0), embeds, 1, 1)
    cross = crosses[:CLASSES] + crosses[CLASSES : 2 * CLASSES] + crosses[2 * CLASSES :]
    norm_e = to_lanes(jnp.sum(wide * wide, axis=1, keepdims=True))
    norm_p = jnp.sum(protos * protos, axis=1, keepdims=True)
    distance = norm_e - 2.0 * cross + norm_p
    scores = -distance * D ** (-0.5)
    masked = jnp.where(classes < ways, scores, -1e30)
    top = jnp.max(masked, axis=0, keepdims=True)
    powers = jnp.exp(masked - top)
    total = jnp.sum(powers, axis=0, keepdims=True)
    picked = jnp.sum(jnp.where(hot, scores, 0.0), axis=0, keepdims=True)
    per_query = jnp.where(query > 0.0, top + jnp.log(total) - picked, 0.0)
    queries = jnp.maximum(jnp.sum(query, axis=1, keepdims=True), 1.0)
    loss = jnp.sum(per_query, axis=1, keepdims=True) / queries
    share = query / queries
    by_dist = (jnp.where(hot, 1.0, 0.0) - powers / total) * (share * D ** (-0.5))
    by_parts = three_parts(by_dist)
    pulls = dot(jnp.concatenate(by_parts, axis=0), embeds, 1, 0)
    pull = pulls[:CLASSES] + pulls[CLASSES : 2 * CLASSES] + pulls[2 * CLASSES :]
    by_sums = 2.0 * (protos * jnp.sum(by_dist, axis=1, keepdims=True) - pull) / counts
    sum_parts = three_parts(by_sums)
    left = jnp.concatenate([by_parts[0], by_parts[0], by_parts[1], support, support], axis=0)
    right = jnp.concatenate(
        [-2.0 * parts[0], -2.0 * parts[1], -2.0 * parts[0], sum_parts[0], sum_parts[1]], axis=0
    )
    own = to_sublanes(jnp.sum(by_dist, axis=0, keepdims=True))
    grads = dot(left, right, 0, 0) + 2.0 * own * wide
    return grads.astype(BF16), loss


def farthest_first(count):
    return sorted(range(count), key=lambda i: -min(i, count - i))


def one_hot(places, count):
    return jnp.where(iota((count, places.shape[1]), 0) == places, 1.0, 0.0).astype(BF16)


def arrived(block, sem):
    pltpu.make_async_copy(block, block, sem).wait()


def lay_out(blocks, out_ref, which):
    lines = out_ref.shape[0] // 2
    value = blocks[which].reshape(D // LANES, lines, LANES)
    start = which * lines
    for i in range(D // LANES):
        out_ref[start : start + lines, i * LANES : (i + 1) * LANES] = value[i].astype(F32)


def kernel(
    n,
    n_group,
    owner_hbm,
    slot_hbm,
    query_hbm,
    ways_hbm,
    features_hbm,
    weight_hbm,
    out_rows_ref,
    out_weight_ref,
    out_loss_ref,
    owner_ref,
    slot_ref,
    query_ref,
    ways_ref,
    features_ref,
    weight_ref,
    code_send,
    code_mid,
    code_recv,
    left_send,
    left_mid,
    left_recv,
    right_send,
    right_mid,
    right_recv,
    back_send,
    back_recv,
    halves,
    fold_send,
    fold_recv,
    part_send,
    part_recv,
    line_send,
    line_recv,
    whole,
    load_sem,
    code_ss,
    code_rs,
    left_ss,
    left_rs,
    right_ss,
    right_rs,
    back_ss,
    back_rs,
    pair_ss,
    pair_rs,
    part_ss,
    part_rs,
    line_ss,
    line_rs,
    whole_ss,
    whole_rs,
    tick,
):
    me = lax.axis_index("dp")
    group = lax.axis_index("group")
    chips = n // 2
    side = math.isqrt(chips)
    spots = side * n_group
    core = lax.rem(me, 2)
    chip = lax.div(me, 2)
    high = lax.div(chip, side)
    low = lax.rem(chip, side)
    twin = me + 1 - 2 * core
    rows = features_ref.shape[0]
    half = D // 2
    offsets = farthest_first(side)
    highs = [lax.rem(high + i, side) * (2 * side) for i in range(side)]
    lows = [lax.rem(low + i, side) * 2 for i in range(side)]
    wide = 2 * side
    mine = 2 * low + core
    row_line = [(2 * lax.rem(low + i, side) + c, highs[0] + lows[i] + c) for i in offsets if i for c in range(2)]
    row_line.append((mine + 1 - 2 * core, twin))
    groups = [lax.rem(group + i, n_group) for i in range(1, n_group)]
    plane = [(h, w) for h in offsets for w in offsets if h or w]
    row_peers = [highs[h] + lows[w] + c for h, w in plane for c in range(2)] + [twin]
    lines = [
        (low, [(lax.rem(low + i, side), highs[0] + lows[i] + core) for i in offsets if i]),
        (high, [(lax.rem(high + i, side), highs[i] + lows[0] + core) for i in offsets if i]),
    ]

    barrier = pltpu.get_barrier_semaphore()
    with jax.named_scope("greet"):
        for _, peer in row_line + lines[1][1]:
            pl.semaphore_signal(barrier, inc=1, device_id=(peer, group), device_id_type=MESH)
        for peer in groups:
            pl.semaphore_signal(barrier, inc=1, device_id=(me, peer), device_id_type=MESH)
    pairs = (
        (owner_hbm, owner_ref, 0),
        (slot_hbm, slot_ref, 0),
        (query_hbm, query_ref, 0),
        (features_hbm, features_ref, 1),
        (ways_hbm, ways_ref, 2),
        (weight_hbm, weight_ref, 3),
    )
    loads = [pltpu.make_async_copy(source, target, load_sem.at[i]) for source, target, i in pairs]
    for load in loads:
        load.start()
    arrived(code_mid.at[pl.ds(0, 3)], load_sem.at[0])
    for load in loads[3:]:
        load.wait()

    owner_lane = owner_ref[...].astype(F32)
    owner = to_sublanes(owner_lane)
    earlier = (owner == owner_lane) & (iota((rows, rows), 0) < iota((rows, rows), 1))
    place = jnp.sum(jnp.where(earlier, 1.0, 0.0), axis=0, keepdims=True)
    codes = (slot_ref[...] * 2 + query_ref[...] + 1).astype(F32)
    weighed = to_sublanes(codes * jnp.where(place > 0.0, 1.0 * LANES, 1.0))
    code_send[...] = jnp.sum(
        jnp.where(owner == iota((rows, n), 1).astype(F32), weighed, 0.0), axis=0, keepdims=True
    )
    code_mid[mine] = code_send[...]
    target = owner_lane.astype(I32)
    place = place.astype(I32)
    hot = one_hot(target * CAP + place, n * CAP)
    turned = (lax.rem(target, wide) * side + lax.div(target, wide)) * CAP + place
    left = dot(one_hot(turned, n * CAP), features_ref[:, :half], 1, 0).astype(BF16)
    left_send[...] = left.reshape(left_send.shape)
    right = dot(hot, features_ref[:, half:], 1, 0).astype(BF16)
    right_send[...] = right.reshape(right_send.shape)
    left_mid[:, mine] = left_send[mine]
    right_mid[:, high] = right_send[high]

    with jax.named_scope("barrier_wait"):
        pl.semaphore_wait(barrier, wide + side + n_group - 3)

    def push(source, target, send_sem, recv_sem, peer):
        pltpu.make_async_remote_copy(
            src_ref=source,
            dst_ref=target,
            send_sem=send_sem,
            recv_sem=recv_sem,
            device_id=(peer, group),
            device_id_type=MESH,
        ).start()

    with jax.named_scope("send_rows"):
        for place, peer in row_line:
            push(code_send, code_mid.at[mine], code_ss, code_rs.at[0], peer)
        for place, peer in row_line:
            push(left_send.at[place], left_mid.at[:, mine], left_ss, left_rs.at[0], peer)
        for place, peer in lines[1][1]:
            push(right_send.at[place], right_mid.at[:, high], right_ss, right_rs.at[0], peer)
    with jax.named_scope("code_wait0"):
        arrived(code_mid.at[pl.ds(0, wide - 1)], code_rs.at[0])
    for place, peer in lines[1][1]:
        push(code_mid, code_recv.at[pl.ds(high * wide, wide)], code_ss, code_rs.at[1], peer)
    code_recv[pl.ds(high * wide, wide)] = code_mid[...]
    with jax.named_scope("left_wait0"):
        arrived(left_mid.at[:, pl.ds(0, wide - 1)], left_rs.at[0])
    for place, peer in lines[1][1]:
        push(left_mid.at[place], left_recv.at[high], left_ss, left_rs.at[1], peer)
    left_recv[high] = left_mid[high]
    with jax.named_scope("right_wait0"):
        arrived(right_mid.at[:, pl.ds(0, side - 1)], right_rs.at[0])
    for place, peer in row_line:
        push(right_mid.at[place], right_recv.at[:, mine], right_ss, right_rs.at[1], peer)
    right_recv[:, mine] = right_mid[mine]
    with jax.named_scope("code_wait1"):
        arrived(code_recv.at[pl.ds(0, n - wide)], code_rs.at[1])
    table = code_recv[...].reshape(n, n)
    both = jnp.sum(jnp.where(iota((n, n), 1) == me, table, 0.0), axis=1, keepdims=True).astype(I32)
    spot = iota((n, n * CAP), 1)
    chosen = jnp.where(lax.rem(spot, CAP) == 0, lax.rem(both, LANES), lax.div(both, LANES))
    chosen = jnp.where(lax.div(spot, CAP) == iota((n, n * CAP), 0), chosen, 0)
    got_codes = jnp.sum(chosen.astype(F32), axis=0, keepdims=True)
    with jax.named_scope("left_wait1"):
        arrived(left_recv.at[pl.ds(0, side - 1)], left_rs.at[1])
    halves[0] = left_recv[...].reshape(n * CAP, half)
    with jax.named_scope("right_wait1"):
        arrived(right_recv.at[:, pl.ds(0, wide - 1)], right_rs.at[1])
    halves[1] = right_recv[...].reshape(n * CAP, half)
    got_rows = jnp.concatenate([halves[0], halves[1]], axis=1)
    with jax.named_scope("episode"):
        grads, loss = episode(got_rows, got_codes, ways_ref[...], weight_ref[...])
        out_loss_ref[...] = loss

    def term(which):
        value = dot(halves[which], grads, 0, 0)
        return jnp.concatenate(
            [value[:, i * LANES : (i + 1) * LANES] for i in range(D // LANES)], axis=0
        )

    def fold(which):
        return pltpu.make_async_remote_copy(
            src_ref=fold_send.at[which],
            dst_ref=fold_recv.at[which],
            send_sem=pair_ss,
            recv_sem=pair_rs.at[which],
            device_id=(twin, group),
            device_id_type=MESH,
        )

    def last(which):
        return pltpu.make_async_remote_copy(
            src_ref=whole.at[which],
            dst_ref=whole.at[which],
            send_sem=pair_ss,
            recv_sem=pair_rs.at[which],
            device_id=(twin, group),
            device_id_type=MESH,
        )

    def prepare_back():
        outgoing = dot(grads, weight_ref[...], 1, 1).astype(BF16)
        back_send[...] = outgoing.reshape(back_send.shape)
        back_recv[me] = back_send[me]

    def send_back(which, piece):
        with jax.named_scope(f"send_back{piece}"):
            for peer in row_peers[BACK[which][piece] : BACK[which][piece + 1]]:
                push(back_send.at[peer], back_recv.at[me], back_ss, back_rs, peer)

    def take_back():
        with jax.named_scope("back_wait"):
            arrived(back_recv.at[pl.ds(0, n - 1)], back_rs)
        returned = back_recv[...].reshape(n * CAP, D)
        out_rows_ref[...] = dot(hot, returned, 0, 0).astype(BF16)

    def spread(axis, source, target, send_sem, recv_sem):
        places = lines[axis][1] + [(lines[axis][0], me)]
        shifts = [i for i in offsets if i] + [0]
        pairs = [(p, g) for p in range(side) for g in range(n_group) if shifts[p] or g]
        hops = lambda i, count: min(i, count - i)
        pairs.sort(key=lambda pair: -hops(shifts[pair[0]], side) - hops(pair[1], n_group))
        for p, g in pairs:
            place, peer = places[p]
            other = ([group] + groups)[g]
            pltpu.make_async_remote_copy(
                src_ref=source(place, other),
                dst_ref=target,
                send_sem=send_sem,
                recv_sem=recv_sem,
                device_id=(peer, other),
                device_id_type=MESH,
            ).start()

    def tell():
        pl.semaphore_signal(tick, inc=1, device_id=(twin, group), device_id_type=MESH)

    @pl.when(core == 1)
    def _():
        own = [term(0), term(1)]
        prepare_back()
        for i in range(2):
            with jax.named_scope(f"fold_wait{i}"):
                fold(i).wait_recv()
            total = own[i] + fold_recv[i].astype(F32)
            part_send[i] = total.astype(BF16).reshape(part_send.shape[1:])
            here = lines[i][0] * n_group + group
            spread(i, lambda p, g: part_send.at[i, p * n_group + g], part_recv.at[i, here], part_ss, part_rs.at[i])
            part_recv[i, here] = part_send[i, here]
        for i in range(2):
            with jax.named_scope(f"part_wait{i}"):
                arrived(part_recv.at[i, pl.ds(0, spots - 1)], part_rs.at[i])
            line_send[i] = jnp.sum(part_recv[i].astype(F32), axis=0).astype(BF16)
            here = lines[1 - i][0]
            for _, peer in lines[1 - i][1]:
                push(line_send.at[i], line_recv.at[i, here], line_ss, line_rs.at[i], peer)
            line_recv[i, here] = line_send[i]
        tell()
        send_back(1, 0)
        for i in range(2):
            with jax.named_scope(f"line_wait{i}"):
                arrived(line_recv.at[i, pl.ds(0, side - 1)], line_rs.at[i])
            here = lines[i][0] * n_group + group
            whole[i, here] = jnp.sum(line_recv[i].astype(F32), axis=0).astype(BF16)
            final = whole.at[i, here]
            spread(i, lambda p, g: final, final, whole_ss, whole_rs.at[i])
        for i in range(2):
            with jax.named_scope(f"whole_wait{i}"):
                arrived(whole.at[i, pl.ds(0, spots - 1)], whole_rs.at[i])
            last(i).start()
        for i in range(2):
            lay_out(whole, out_weight_ref, i)
        take_back()
        arrived(part_recv.at[:, pl.ds(0, spots - 1)], part_ss)
        arrived(line_recv.at[:, pl.ds(0, side - 1)], line_ss)
        arrived(whole.at[:, pl.ds(0, spots - 1)], whole_ss)
        arrived(whole, pair_ss)

    @pl.when(core == 0)
    def _():
        for i in range(2):
            fold_send[i] = term(i).astype(BF16)
            fold(i).start()
        prepare_back()
        if WAIT[0]:
            pl.delay(WAIT[0])
        send_back(0, 0)
        with jax.named_scope("tick_wait"):
            pl.semaphore_wait(tick, 1)
        if WAIT[1]:
            pl.delay(WAIT[1])
        send_back(0, 1)
        take_back()
        for i in range(2):
            with jax.named_scope(f"last_wait{i}"):
                last(i).wait_recv()
            lay_out(whole, out_weight_ref, i)
        arrived(fold_send, pair_ss)

    arrived(code_recv.at[pl.ds(0, n - 1)], code_ss)
    sent = ((wide - 1) * side + (side - 1) * wide) // 2
    arrived(back_send.at[pl.ds(0, sent)], left_ss)
    arrived(back_send.at[pl.ds(0, sent)], right_ss)
    arrived(back_send.at[pl.ds(0, n - 1)], back_ss)


def put_out(rows_ref, terms_ref, loss_ref, out_rows, out_terms, out_loss, sems):
    pieces = 8
    lines = terms_ref.shape[0] // pieces
    for i in range(pieces):
        block = pl.ds(i * lines, lines)
        pltpu.make_async_copy(terms_ref.at[block], out_terms.at[block], sems.at[0]).start()
    others = [
        pltpu.make_async_copy(rows_ref, out_rows, sems.at[1]),
        pltpu.make_async_copy(loss_ref, out_loss, sems.at[2]),
    ]
    for copy in others:
        copy.start()
    arrived(terms_ref, sems.at[0])
    for copy in others:
        copy.wait()


def on_device(n, n_group, features, weight, owner, slots, queries, ways):
    rows = features.shape[0]
    chips = n // 2
    lines = D * D // LANES
    vmem = pl.BlockSpec(memory_space=pltpu.VMEM)
    dma = pltpu.SemaphoreType.DMA
    two = pltpu.SemaphoreType.DMA((2,))
    side = math.isqrt(chips)
    part = (2, side * n_group, lines // (2 * side * n_group), LANES)
    hbm = pl.BlockSpec(memory_space=pl.ANY)
    own_rows, terms, losses = pl.pallas_call(
        functools.partial(kernel, n, n_group),
        out_shape=(
            pltpu.VMEM((rows, D), BF16),
            pltpu.VMEM((D, D), F32),
            pltpu.VMEM((1, 1), F32),
        ),
        in_specs=[hbm] * 6,
        out_specs=(vmem, vmem, vmem),
        scratch_shapes=[
            pltpu.VMEM((1, rows), I32),
            pltpu.VMEM((1, rows), I32),
            pltpu.VMEM((1, rows), I32),
            pltpu.VMEM((1, 1), I32),
            pltpu.VMEM((rows, D), BF16),
            pltpu.VMEM((D, D), BF16),
            pltpu.VMEM((1, n), F32),
            pltpu.VMEM((2 * side, 1, n), F32),
            pltpu.VMEM((n, 1, n), F32),
            pltpu.VMEM((2 * side, side, CAP, D // 2), BF16),
            pltpu.VMEM((side, 2 * side, CAP, D // 2), BF16),
            pltpu.VMEM((side, 2 * side, CAP, D // 2), BF16),
            pltpu.VMEM((side, 2 * side, CAP, D // 2), BF16),
            pltpu.VMEM((2 * side, side, CAP, D // 2), BF16),
            pltpu.VMEM((side, 2 * side, CAP, D // 2), BF16),
            pltpu.VMEM((n, CAP, D), BF16),
            pltpu.VMEM((n, CAP, D), BF16),
            pltpu.VMEM((2, n * CAP, D // 2), BF16),
            pltpu.VMEM((2, lines // 2, LANES), BF16),
            pltpu.VMEM((2, lines // 2, LANES), BF16),
            pltpu.VMEM(part, BF16),
            pltpu.VMEM(part, BF16),
            pltpu.VMEM((2, *part[2:]), BF16),
            pltpu.VMEM((2, side, *part[2:]), BF16),
            pltpu.VMEM(part, BF16),
            pltpu.SemaphoreType.DMA((4,)),
        ]
        + [dma, two] * 3
        + [dma, dma]
        + [dma, two] * 4
        + [pltpu.SemaphoreType.REGULAR],
        compiler_params=pltpu.CompilerParams(collective_id=0, has_side_effects=True),
        name="episodes",
    )(
        owner.reshape(1, rows),
        slots.reshape(1, rows),
        queries.reshape(1, rows),
        ways.reshape(1, 1),
        features,
        weight,
    )
    own_rows, terms, losses = pl.pallas_call(
        put_out,
        out_shape=(
            jax.ShapeDtypeStruct((rows, D), BF16),
            jax.ShapeDtypeStruct((D, D), F32),
            jax.ShapeDtypeStruct((1, 1), F32),
        ),
        in_specs=[vmem] * 3,
        out_specs=(hbm, hbm, hbm),
        scratch_shapes=[pltpu.SemaphoreType.DMA((3,))],
        name="results",
    )(*(pltpu.with_memory_space_constraint(x, pltpu.VMEM) for x in (own_rows, terms, losses)))
    return own_rows, terms, losses.reshape(1)


def solution(mesh):
    both = P(("dp", "group"))
    lines = P(("dp", "group"), None)
    return jax.shard_map(
        functools.partial(on_device, mesh.shape["dp"], mesh.shape["group"]),
        mesh=mesh,
        in_specs=(lines, P(), lines, both, both, both),
        out_specs=(lines, P(), both),
        check_vma=False,
    )
```
